32 devices in a mesh: dp: 2 (over x), fsdp: 16 (over z, y, core).
Axes of the slice: x: 2, y: 2, z: 4, core: 2. Of those that a mesh axis runs over, the one named last changes fastest.
Arguments:
- inputs: bfloat16 [32, 512, 768], P(('dp', 'fsdp')), may hold values from -6 to 6
- segments: int32 [32, 512], P(('dp', 'fsdp')), may hold values from 0 to 3, never falling along the last dimension, each value on 1 to 256 neighbouring positions
- out_grads: bfloat16 [4, 32, 512, 768], P(None, ('dp', 'fsdp')), may hold values from -6 to 6
- query_weight: bfloat16 [768, 768], P(('dp', 'fsdp')), may hold values from -0.21875 to 0.21875
- query_bias: bfloat16 [768], P(('dp', 'fsdp')), may hold values from -1.1953125 to 1.1953125
- key_weight: bfloat16 [768, 768], P(('dp', 'fsdp')), may hold values from -0.21875 to 0.21875
- value_weight: bfloat16 [768, 768], P(('dp', 'fsdp')), may hold values from -0.21875 to 0.21875
- value_bias: bfloat16 [768], P(('dp', 'fsdp')), may hold values from -1.1953125 to 1.1953125
- output_weight: bfloat16 [768, 768], P(('dp', 'fsdp')), may hold values from -2.5 to 2.5
- output_bias: bfloat16 [768], P(('dp', 'fsdp')), may hold values from -1.1953125 to 1.1953125
- first_gain: bfloat16 [768], P(('dp', 'fsdp')), may hold values from 0.5 to 1.5
- first_shift: bfloat16 [768], P(('dp', 'fsdp')), may hold values from -1.1953125 to 1.1953125
- inner_weight: bfloat16 [768, 3072], P(('dp', 'fsdp')), may hold values from -0.21875 to 0.21875
- inner_bias: bfloat16 [3072], P(('dp', 'fsdp')), may hold values from -1.1953125 to 1.1953125
- outer_weight: bfloat16 [3072, 768], P(('dp', 'fsdp')), may hold values from -0.21875 to 0.21875
- outer_bias: bfloat16 [768], P(('dp', 'fsdp')), may hold values from -1.1953125 to 1.1953125
- second_gain: bfloat16 [768], P(('dp', 'fsdp')), may hold values from 0.5 to 1.5
- second_shift: bfloat16 [768], P(('dp', 'fsdp')), may hold values from -1.1953125 to 1.1953125
Outputs:
- outputs: bfloat16 [4, 32, 512, 768], P(None, ('dp', 'fsdp'))
- input_grad: float32 [32, 512, 768], P(('dp', 'fsdp'))
- query_weight_grad: float32 [768, 768], P(('dp', 'fsdp'))
- query_bias_grad: float32 [768], P(('dp', 'fsdp'))
- key_weight_grad: float32 [768, 768], P(('dp', 'fsdp'))
- value_weight_grad: float32 [768, 768], P(('dp', 'fsdp'))
- value_bias_grad: float32 [768], P(('dp', 'fsdp'))
- output_weight_grad: float32 [768, 768], P(('dp', 'fsdp'))
- output_bias_grad: float32 [768], P(('dp', 'fsdp'))
- first_gain_grad: float32 [768], P(('dp', 'fsdp'))
- first_shift_grad: float32 [768], P(('dp', 'fsdp'))
- inner_weight_grad: float32 [768, 3072], P(('dp', 'fsdp'))
- inner_bias_grad: float32 [3072], P(('dp', 'fsdp'))
- outer_weight_grad: float32 [3072, 768], P(('dp', 'fsdp'))
- outer_bias_grad: float32 [768], P(('dp', 'fsdp'))
- second_gain_grad: float32 [768], P(('dp', 'fsdp'))
- second_shift_grad: float32 [768], P(('dp', 'fsdp'))
The draws below stay inside these ranges and needn't reach their ends.
Inputs may be any that keep to these rules, and one draw needn't show every extreme that they name: `segments`: in each row the segment numbers start at 0, never fall, and each of the 4 examples holds 1 to 256 tokens.
All inputs are finite; a program needn't handle non-finite values.
Results may differ from the reference program's by a relative error of at most 0.014.
Values may be sent and summed in bfloat16 or wider, within the bound.
A program may use at most 256 MiB of HBM per device.

```python
import math
import jax
import jax.numpy as jnp
import numpy as np
from jax import lax

D = 768
HEADS = 12
DH = 64
FF = 3072
WIDTHS = 4
EXAMPLES = 4
SEQ = 512
DA = 768
ROWS = 32


def spiked(array, stream_key, source, target, blocks, factor):
    def block_of(axis_at):
        return (jnp.arange(array.shape[axis_at]) // (array.shape[axis_at] // blocks)).reshape((-1,) + (1,) * (array.ndim - 1 - axis_at))

    one_side = jax.random.permutation(stream_key, blocks)[block_of(target)]
    far = (block_of(target) + blocks // 2) % blocks
    return jnp.where((block_of(source) == one_side) | (block_of(source) == far), factor * array, array)


def shard_levels(rng, extent, shards, smallest, high):
    loudness, own = 1.0, jax.random.fold_in(rng, 6)
    for dim, parts in shards:
        steps = jnp.exp(jax.random.uniform(jax.random.fold_in(own, dim), (parts,), jnp.float32, smallest / len(shards), high / len(shards)))
        loudness = loudness * jnp.repeat(steps, extent[dim] // parts).reshape([-1 if axis == dim else 1 for axis in range(len(extent))])
    return loudness


def split_up(count, total, limit, skew):
    weights = [(1 << 20) // math.isqrt(rank ** skew) + 1 for rank in range(2, count + 1)]
    surplus, given = total - limit - (count - 1), [1] * (count - 1)
    while surplus > 0:
        candidates = [i for i in range(count - 1) if given[i] < limit]
        mass, left = sum([weights[i] for i in candidates]), surplus
        for i in candidates:
            more = min(limit - given[i], max(1, left * weights[i] // mass), surplus)
            given[i] = given[i] + more
            surplus = surplus - more
    return np.array([limit] + given)


def ragged_sizes(own_key, amount, total, bound, lean):
    if amount == 2:
        one = jax.random.randint(own_key, (), max(1, total - bound), min(bound, total - 1) + 1)
        return jnp.stack([one, total - one])
    tallies = jnp.asarray(split_up(amount, total, bound, lean), jnp.int32)
    pairs = (amount - 1) // 2
    giver, receiver = tallies[1:1 + 2 * pairs:2], tallies[2:2 + 2 * pairs:2]
    slack = jnp.minimum(giver - 1, bound - receiver)
    moved = jax.random.randint(jax.random.fold_in(own_key, 1), (pairs,), 0, 1 << 20) % (slack + 1)
    tallies = tallies.at[1:1 + 2 * pairs:2].set(giver - moved).at[2:2 + 2 * pairs:2].set(receiver + moved)
    return tallies[jax.random.permutation(jax.random.fold_in(own_key, 2), amount)]


def noise(own_key, shape, scale, reach, split=(), dtype=jnp.bfloat16):
    loudness = shard_levels(own_key, shape, split, -0.22, 0.18) if split else 1.0
    drawn = jax.random.normal(own_key, shape, jnp.float32) * scale * loudness
    return jnp.minimum(jnp.maximum(drawn, -reach), reach).astype(dtype)


def heavy_noise(key, shape, spread, bound, split, heavy, kind=jnp.bfloat16):
    entries = spread * jax.random.normal(key, shape, jnp.float32)
    if split:
        entries = entries * shard_levels(key, shape, split, -0.22, 0.18)
    return jnp.clip(spiked(entries, jax.random.fold_in(key, 3), *heavy), -bound, bound).astype(kind)


def setup_inputs(seed: int = 0) -> dict:
    seeds = jax.random.split(jax.random.key(seed), 19)
    inputs = noise(seeds[0], (ROWS, SEQ, D), 1.0, 6.0, ((0, 32),))
    segments = jax.vmap(lambda own: jnp.searchsorted(jnp.cumsum(ragged_sizes(own, EXAMPLES, SEQ, SEQ // 2, 1)), jnp.arange(SEQ), side="right"))(jax.random.split(seeds[1], ROWS)).reshape((ROWS, SEQ)).astype(jnp.int32)
    out_grads = heavy_noise(seeds[2], (WIDTHS, ROWS, SEQ, D), 1.0, 6.0, ((1, 32),), (1, 3, 32, 2.75))
    query_weight = noise(seeds[3], (D, DA), D ** -0.5, 0.21875, ((0, 32),))
    query_bias = noise(seeds[4], (DA,), 0.3, 1.1953125, ((0, 32),))
    key_weight = noise(seeds[5], (D, DA), D ** -0.5, 0.21875, ((0, 32),))
    value_weight = noise(seeds[6], (D, DA), D ** -0.5, 0.21875, ((0, 32),))
    value_bias = noise(seeds[7], (DA,), 0.3, 1.1953125, ((0, 32),))
    output_weight = noise(seeds[8], (DA, D), (DA // 128) ** -0.5, 2.5, ((0, 32),))
    output_bias = noise(seeds[9], (D,), 0.3, 1.1953125, ((0, 32),))
    first_gain = jnp.clip(1.0 + 0.1 * jax.random.normal(seeds[10], (D,), jnp.float32), 0.5, 1.5).astype(jnp.bfloat16)
    first_shift = noise(seeds[11], (D,), 0.3, 1.1953125, ((0, 32),))
    inner_weight = noise(seeds[12], (D, FF), D ** -0.5, 0.21875, ((0, 32),))
    inner_bias = noise(seeds[13], (FF,), 0.3, 1.1953125, ((0, 32),))
    outer_weight = noise(seeds[14], (FF, D), (FF // 4) ** -0.5, 0.21875, ((0, 32),))
    outer_bias = noise(seeds[15], (D,), 0.3, 1.1953125, ((0, 32),))
    second_gain = jnp.clip(1.0 + 0.1 * jax.random.normal(seeds[16], (D,), jnp.float32), 0.5, 1.5).astype(jnp.bfloat16)
    second_shift = noise(seeds[17], (D,), 0.3, 1.1953125, ((0, 32),))
    return dict(inputs=inputs, segments=segments, out_grads=out_grads, query_weight=query_weight, query_bias=query_bias, key_weight=key_weight, value_weight=value_weight, value_bias=value_bias, output_weight=output_weight, output_bias=output_bias, first_gain=first_gain, first_shift=first_shift, inner_weight=inner_weight, inner_bias=inner_bias, outer_weight=outer_weight, outer_bias=outer_bias, second_gain=second_gain, second_shift=second_shift)


EPSILON = 1e-12
SCORE_SCALE = 0.125
MASKED = -1000000000.0

@jax.custom_vjp
def low(v):
    return lax.optimization_barrier(v.astype(jnp.bfloat16)).astype(jnp.float32)

@jax.custom_vjp
def low_back(v):
    return v

def low_keep(v):
    return (low(v), None)

def low_pass(kept, grad):
    return (grad,)

def back_keep(v):
    return (v, None)

def back_low(kept, grad):
    return (low(grad),)
low.defvjp(low_keep, low_pass)
low_back.defvjp(back_keep, back_low)

def matmul_high(left, right):
    return jnp.dot(left, right, precision=lax.Precision.HIGHEST)

def layer_norm(hidden, gain, shift):
    center = hidden - lax.optimization_barrier(jnp.mean(hidden, axis=-1, keepdims=True))
    scaled = center * lax.rsqrt(lax.optimization_barrier(jnp.mean(center * center, axis=-1, keepdims=True)) + EPSILON)
    return scaled * gain + shift

def split_heads(values, head_count):
    return values.reshape(SEQ, head_count, DH).transpose(1, 0, 2)

def forward(weight_set, row_vals, same_seg):
    query_weight, query_bias, key_weight, value_weight, value_bias, output_weight, output_bias, first_gain, first_shift, inner_weight, inner_bias, outer_weight, outer_bias, second_gain, second_shift = weight_set

    def one_head(packed):
        query_rows, key_rows, value_rows = packed
        scores = low_back(jnp.einsum('qd,kd->qk', query_rows, key_rows, precision=lax.Precision.HIGHEST) * SCORE_SCALE)
        scores = jnp.where(same_seg, scores, MASKED)
        attn_probs = low(jax.nn.softmax(scores, axis=-1))
        return matmul_high(attn_probs, value_rows)
    results = []
    for multiple in range(1, WIDTHS + 1):
        head_count = HEADS * multiple // WIDTHS
        feat_width = head_count * DH
        hidden = FF * multiple // WIDTHS
        queries = low(low_back(matmul_high(row_vals, query_weight[:, :feat_width]) + query_bias[:feat_width]))
        key_vals = low(low_back(matmul_high(row_vals, key_weight[:, :feat_width])))
        values = low(low_back(matmul_high(row_vals, value_weight[:, :feat_width]) + value_bias[:feat_width]))
        head_outs = lax.map(jax.checkpoint(one_head), (split_heads(queries, head_count), split_heads(key_vals, head_count), split_heads(values, head_count)))
        attended = low(low_back(head_outs.transpose(1, 0, 2).reshape(SEQ, feat_width)))
        branch = low_back(matmul_high(attended, output_weight[:feat_width]) + output_bias)
        first_out = layer_norm(row_vals + branch, first_gain, first_shift)
        inner_pre = low_back(matmul_high(low(first_out), inner_weight[:, :hidden]) + inner_bias[:hidden])
        activated = low(jax.nn.gelu(inner_pre, approximate=False))
        outer_out = low_back(matmul_high(activated, outer_weight[:hidden]) + outer_bias)
        results.append(layer_norm(first_out + outer_out, second_gain, second_shift))
    return jnp.stack(results)

def reference(inputs, segments, out_grads, query_weight, query_bias, key_weight, value_weight, value_bias, output_weight, output_bias, first_gain, first_shift, inner_weight, inner_bias, outer_weight, outer_bias, second_gain, second_shift):
    params = tuple((weight_array.astype(jnp.float32) for weight_array in (query_weight, query_bias, key_weight, value_weight, value_bias, output_weight, output_bias, first_gain, first_shift, inner_weight, inner_bias, outer_weight, outer_bias, second_gain, second_shift)))

    def row_step(totals, packed):
        row_in, row_seg, row_grad = packed
        same_seg = row_seg[:, None] == row_seg[None, :]
        layer_out, pull_back = jax.vjp(lambda weight_set, row_vals: forward(weight_set, row_vals, same_seg), params, row_in.astype(jnp.float32))
        param_grads, row_input_grad = pull_back(row_grad.astype(jnp.float32))
        totals = tuple((earlier + update for earlier, update in zip(totals, param_grads)))
        return (totals, (layer_out.astype(jnp.bfloat16), row_input_grad))
    zero_grads = tuple((jnp.zeros_like(weight_array) for weight_array in params))
    grad_sums, (layer_outs, input_grads) = lax.scan(row_step, zero_grads, (inputs, segments, jnp.transpose(out_grads, (1, 0, 2, 3))))
    outputs = jnp.transpose(layer_outs, (1, 0, 2, 3))
    return (outputs, input_grads, grad_sums[0], grad_sums[1], grad_sums[2], grad_sums[3], grad_sums[4], grad_sums[5], grad_sums[6], grad_sums[7], grad_sums[8], grad_sums[9], grad_sums[10], grad_sums[11], grad_sums[12], grad_sums[13], grad_sums[14])
```

```python
import functools

import jax
import jax.numpy as jnp
from jax import lax
from jax.experimental import pallas as pl
from jax.experimental.pallas import tpu as pltpu
from jax.sharding import PartitionSpec as P

HEADS = 12
DH = 64
WIDTHS = 4
EPSILON = 1e-12
SCORE_SCALE = 0.125
MASKED = -1000000000.0
BF = jnp.bfloat16
F32 = jnp.float32
AXES = ("dp", "fsdp")
EXTRA = 128


def dot(a, b):
    return jnp.dot(a, b, preferred_element_type=F32)


def dot_tn(a, b):
    return lax.dot_general(a, b, (((0,), (0,)), ((), ())), preferred_element_type=F32)


def dot_nt(a, b):
    return lax.dot_general(a, b, (((1,), (1,)), ((), ())), preferred_element_type=F32)


def attn_fwd_kernel(q_ref, k_ref, v_ref, segc_ref, segr_ref, o_ref, lse_ref):
    q = q_ref[...]
    k = k_ref[...]
    v = v_ref[...]
    lane = lax.broadcasted_iota(jnp.int32, q.shape, 1)
    low = lane < DH
    zero = jnp.zeros_like(q)
    same = segc_ref[...] == segr_ref[...]
    outs = []
    lses = []
    for half in range(2):
        qh = jnp.where(low if half == 0 else ~low, q, zero)
        s = jnp.where(same, dot_nt(qh, k) * SCORE_SCALE, MASKED)
        m = jnp.max(s, axis=-1, keepdims=True)
        e = jnp.exp(s - m)
        total = jnp.sum(e, axis=-1, keepdims=True)
        p = (e * (1.0 / total)).astype(BF)
        outs.append(dot(p, v))
        lses.append(m + jnp.log(total))
    o_ref[...] = jnp.where(low, outs[0], outs[1]).astype(BF)
    lse_ref[...] = jnp.where(low, lses[0], lses[1])


def attn_bwd_kernel(q_ref, k_ref, v_ref, g_ref, segc_ref, segr_ref, lse_ref, dq_ref, dk_ref, dv_ref):
    q = q_ref[...]
    k = k_ref[...]
    v = v_ref[...]
    g = g_ref[...]
    lane = lax.broadcasted_iota(jnp.int32, q.shape, 1)
    low = lane < DH
    zero = jnp.zeros_like(q)
    same = segc_ref[...] == segr_ref[...]
    res = []
    for half in range(2):
        mine = low if half == 0 else ~low
        qh = jnp.where(mine, q, zero)
        gh = jnp.where(mine, g, zero)
        s = jnp.where(same, dot_nt(qh, k) * SCORE_SCALE, MASKED)
        p = jnp.exp(s - lse_ref[:, half * DH : half * DH + 1])
        dp = dot_nt(gh, v)
        ds = (p * (dp - jnp.sum(p * dp, axis=-1, keepdims=True))).astype(BF)
        res.append((dot(ds, k), dot_tn(ds, q), dot_tn(p.astype(BF), g)))
    dq_ref[...] = (jnp.where(low, res[0][0], res[1][0]) * SCORE_SCALE).astype(BF)
    dk_ref[...] = (jnp.where(low, res[0][1], res[1][1]) * SCORE_SCALE).astype(BF)
    dv_ref[...] = jnp.where(low, res[0][2], res[1][2]).astype(BF)


def attn_forward(qkv, segc, segr):
    seq = qkv.shape[0]
    pairs = HEADS // 2
    block = lambda off: pl.BlockSpec((seq, 2 * DH), lambda i: (0, i + off))
    return pl.pallas_call(
        attn_fwd_kernel,
        grid=(pairs,),
        in_specs=[block(0), block(pairs), block(2 * pairs),
                  pl.BlockSpec((seq, 1), lambda i: (0, 0)), pl.BlockSpec((1, seq), lambda i: (0, 0))],
        out_specs=[block(0), block(0)],
        out_shape=[jax.ShapeDtypeStruct((seq, HEADS * DH), BF), jax.ShapeDtypeStruct((seq, HEADS * DH), F32)],
        compiler_params=pltpu.CompilerParams(vmem_limit_bytes=48 << 20),
        name="attn_fwd",
    )(qkv, qkv, qkv, segc, segr)


def attn_backward(qkv, g, segc, segr, lse):
    seq = qkv.shape[0]
    pairs = HEADS // 2
    block = lambda off: pl.BlockSpec((seq, 2 * DH), lambda i: (0, i + off))
    out = jax.ShapeDtypeStruct((seq, HEADS * DH), BF)
    return pl.pallas_call(
        attn_bwd_kernel,
        grid=(pairs,),
        in_specs=[block(0), block(pairs), block(2 * pairs), block(0),
                  pl.BlockSpec((seq, 1), lambda i: (0, 0)), pl.BlockSpec((1, seq), lambda i: (0, 0)), block(0)],
        out_specs=[block(0)] * 3,
        out_shape=[out] * 3,
        compiler_params=pltpu.CompilerParams(vmem_limit_bytes=48 << 20),
        name="attn_bwd",
    )(qkv, qkv, qkv, g, segc, segr, lse)


def normalize(hidden):
    center = hidden - jnp.mean(hidden, axis=-1, keepdims=True)
    inverse = lax.rsqrt(jnp.mean(center * center, axis=-1, keepdims=True) + EPSILON)
    return center * inverse, inverse


def norm_back(upstream, scaled, inverse, gain):
    tg = upstream * gain
    return inverse * (tg - jnp.mean(tg, axis=-1, keepdims=True) - scaled * jnp.mean(tg * scaled, axis=-1, keepdims=True))


def gelu_parts(x):
    phi = 0.5 * (1.0 + lax.erf(x * 0.7071067811865476))
    slope = phi + x * (jnp.exp(-0.5 * x * x) * 0.3989422804014327)
    return (x * phi).astype(BF), slope.astype(BF)


def per_device(inputs, segments, out_grads, wq, bq, wk, wv, bv, wo, bo, g1, s1, wi, bi, wu, bu, g2, s2):
    rows = wq.shape[0]
    dim = wq.shape[1]
    ff = wi.shape[1]
    feat = dim // WIDTHS
    hid = ff // WIDTHS
    small = jnp.concatenate(
        [jnp.stack([bq, bv, bo, g1, s1, bu, g2, s2], axis=1), bi.reshape(rows, ff // dim)], axis=1
    )
    nsmall = small.shape[1]
    small = jnp.pad(small, ((0, 0), (0, EXTRA - nsmall)))
    packed = jnp.concatenate([wq, wk, wv, wo, wi, wu.reshape(rows, ff), small], axis=1)
    full = lax.all_gather(packed, AXES, axis=0, tiled=True)
    wqkv = full[:, : 3 * dim]
    wo_f = full[:, 3 * dim : 4 * dim]
    wi_f = full[:, 4 * dim : 4 * dim + ff]
    wu_f = full[:, 4 * dim + ff : 4 * dim + 2 * ff].reshape(ff, dim)
    sm = full[:, 4 * dim + 2 * ff :].astype(F32)
    vec = sm[:, :8].T
    bq_f, bv_f, bo_f, g1_f, s1_f, bu_f, g2_f, s2_f = [vec[i] for i in range(8)]
    bi_f = sm[:, 8 : 8 + ff // dim].reshape(ff)

    x = inputs[0]
    xf = x.astype(F32)
    seg = segments[0]
    segc, segr = seg[:, None], seg[None, :]
    bqkv = jnp.concatenate([bq_f, jnp.zeros_like(bq_f), bv_f])
    qkv = (dot(x, wqkv) + bqkv).astype(BF)
    att, lse = attn_forward(qkv, segc, segr)

    branch = jnp.zeros(x.shape, F32)
    outs = []
    acts = []
    slopes = []
    lows = []
    back = []
    for k in range(WIDTHS):
        branch = branch + dot(att[:, feat * k : feat * (k + 1)], wo_f[feat * k : feat * (k + 1)])
        scaled1, inv1 = normalize(xf + branch + bo_f)
        first = scaled1 * g1_f + s1_f
        low = first.astype(BF)
        pre = dot(low, wi_f[:, : hid * (k + 1)]) + bi_f[: hid * (k + 1)]
        act, slope = gelu_parts(pre)
        scaled2, inv2 = normalize(first + dot(act, wu_f[: hid * (k + 1)]) + bu_f)
        outs.append((scaled2 * g2_f + s2_f).astype(BF))
        back.append((scaled1, inv1, scaled2, inv2))
        lows.append(low)
        acts.append(act)
        slopes.append(slope)

    obs = []
    ibs = []
    ab_suffix = [None] * WIDTHS
    d_g1 = d_s1 = d_g2 = d_s2 = d_bu = jnp.zeros((dim,), F32)
    bbs = []
    attn_total = jnp.zeros(x.shape, F32)
    for k in range(WIDTHS):
        scaled1, inv1, scaled2, inv2 = back[k]
        up = out_grads[k, 0].astype(F32)
        d_g2 = d_g2 + jnp.sum(up * scaled2, axis=0)
        d_s2 = d_s2 + jnp.sum(up, axis=0)
        sb = norm_back(up, scaled2, inv2, g2_f)
        ob = sb.astype(BF)
        d_bu = d_bu + jnp.sum(ob, axis=0, dtype=F32)
        ib = (dot_nt(ob, wu_f[: hid * (k + 1)]) * slopes[k].astype(F32)).astype(BF)
        fb = sb + dot_nt(ib, wi_f[:, : hid * (k + 1)])
        d_g1 = d_g1 + jnp.sum(fb * scaled1, axis=0)
        d_s1 = d_s1 + jnp.sum(fb, axis=0)
        ab = norm_back(fb, scaled1, inv1, g1_f)
        attn_total = attn_total + ab
        bbs.append(ab)
        obs.append(ob)
        ibs.append(ib)
    suffix = None
    for k in range(WIDTHS - 1, -1, -1):
        suffix = bbs[k] if suffix is None else suffix + bbs[k]
        ab_suffix[k] = suffix.astype(BF)
    d_bo = jnp.sum(attn_total, axis=0)
    d_wo = jnp.concatenate(
        [dot_tn(att[:, feat * k : feat * (k + 1)], ab_suffix[k]) for k in range(WIDTHS)], axis=0
    )
    att_back = jnp.concatenate(
        [dot_nt(ab_suffix[k], wo_f[feat * k : feat * (k + 1)]) for k in range(WIDTHS)], axis=1
    ).astype(BF)

    d_wi = []
    d_wu = []
    d_bi = []
    for j in range(WIDTHS):
        cols = slice(hid * j, hid * (j + 1))
        ib_j = jnp.concatenate([ibs[k][:, cols] for k in range(j, WIDTHS)], axis=0)
        act_j = jnp.concatenate([acts[k][:, cols] for k in range(j, WIDTHS)], axis=0)
        low_j = jnp.concatenate(lows[j:], axis=0)
        ob_j = jnp.concatenate(obs[j:], axis=0)
        d_wi.append(dot_tn(low_j, ib_j))
        d_wu.append(dot_tn(act_j, ob_j))
        d_bi.append(jnp.sum(ib_j, axis=0, dtype=F32))
    d_wi = jnp.concatenate(d_wi, axis=1)
    d_wu = jnp.concatenate(d_wu, axis=0)
    d_bi = jnp.concatenate(d_bi)

    dq, dk, dv = attn_backward(qkv, att_back, segc, segr, lse)
    dqkv = jnp.concatenate([dq, dk, dv], axis=1)
    d_wqkv = dot_tn(x, dqkv)
    x_grad = attn_total + dot_nt(dqkv, wqkv)
    d_bq = jnp.sum(dq, axis=0, dtype=F32)
    d_bv = jnp.sum(dv, axis=0, dtype=F32)

    d_small = jnp.concatenate(
        [jnp.stack([d_bq, d_bv, d_bo, d_g1, d_s1, d_bu, d_g2, d_s2], axis=1), d_bi.reshape(dim, ff // dim)], axis=1
    )
    d_small = jnp.pad(d_small, ((0, 0), (0, EXTRA - nsmall)))
    d_packed = jnp.concatenate(
        [d_wqkv.astype(BF), d_wo.astype(BF), d_wi.astype(BF), d_wu.astype(BF).reshape(dim, ff), d_small.astype(BF)],
        axis=1,
    )
    red = lax.psum_scatter(d_packed, AXES, scatter_dimension=0, tiled=True).astype(F32)
    rs = red[:, 4 * dim + 2 * ff :]
    vecs = [rs[:, i] for i in range(8)]
    r_bi = rs[:, 8 : 8 + ff // dim].reshape(-1)
    return (
        jnp.stack(outs)[:, None],
        x_grad[None],
        red[:, :dim],
        vecs[0],
        red[:, dim : 2 * dim],
        red[:, 2 * dim : 3 * dim],
        vecs[1],
        red[:, 3 * dim : 4 * dim],
        vecs[2],
        vecs[3],
        vecs[4],
        red[:, 4 * dim : 4 * dim + ff],
        r_bi,
        red[:, 4 * dim + ff : 4 * dim + 2 * ff].reshape(-1, dim),
        vecs[5],
        vecs[6],
        vecs[7],
    )


def solution(mesh):
    mat = P(AXES, None)
    vec = P(AXES)
    params = (mat, vec, mat, mat, vec, mat, vec, vec, vec, mat, vec, mat, vec, vec, vec)
    return jax.shard_map(
        per_device,
        mesh=mesh,
        in_specs=(P(AXES, None, None), P(AXES, None), P(None, AXES, None, None)) + params,
        out_specs=(P(None, AXES, None, None), P(AXES, None, None)) + params,
        check_vma=False,
    )
```

```python
import functools

import jax
import jax.numpy as jnp
from jax import lax
from jax.experimental import pallas as pl
from jax.experimental.pallas import tpu as pltpu
from jax.sharding import PartitionSpec as P

HEADS = 12
DH = 64
WIDTHS = 4
EPSILON = 1e-12
SCORE_SCALE = 0.125
MASKED = -1000000000.0
BF = jnp.bfloat16
F32 = jnp.float32
AXES = ("dp", "fsdp")
EXTRA = 128


def dot(a, b):
    return jnp.dot(a, b, preferred_element_type=F32)


def dot_tn(a, b):
    return lax.dot_general(a, b, (((0,), (0,)), ((), ())), preferred_element_type=F32)


def dot_nt(a, b):
    return lax.dot_general(a, b, (((1,), (1,)), ((), ())), preferred_element_type=F32)


MESH = pl.DeviceIdType.MESH


class Place:
    def __init__(self):
        self.x = lax.axis_index("dp")
        f = lax.axis_index("fsdp")
        self.z = f // 4
        self.y = (f // 2) % 2
        self.c = f % 2

    def ident(self, x=None, z=None, y=None, c=None):
        x = self.x if x is None else x
        z = self.z if z is None else z
        y = self.y if y is None else y
        c = self.c if c is None else c
        return {"dp": x, "fsdp": z * 4 + y * 2 + c}

    def index(self, x=None, z=None, y=None, c=None):
        x = self.x if x is None else x
        z = self.z if z is None else z
        y = self.y if y is None else y
        c = self.c if c is None else c
        return x * 16 + z * 4 + y * 2 + c


def greet(place):
    barrier = pltpu.get_barrier_semaphore()
    others = [place.ident(z=lax.rem(place.z + o, 4)) for o in (1, 2, 3)]
    others += [place.ident(x=1 - place.x), place.ident(y=1 - place.y), place.ident(c=1 - place.c)]
    for other in others:
        pl.semaphore_signal(barrier, inc=1, device_id=other, device_id_type=MESH)
    pl.semaphore_wait(barrier, len(others))


def chunk_list(parts, order_first):
    return parts


def gather_kernel(chunks, ins, outs, send_sem, recv_sem, own_sem):
    place = Place()
    greet(place)
    me = place.index()
    counts = [0] * len(chunks)

    def mine(ci):
        a, rows, r0, nr, c0, nc, order = chunks[ci]
        return ins[a].at[pl.ds(r0, nr), pl.ds(c0, nc)]

    def slot(ci, shard):
        a, rows, r0, nr, c0, nc, order = chunks[ci]
        return outs[a].at[pl.ds(pl.multiple_of(shard * rows + r0, 8), nr), pl.ds(c0, nc)]

    pending = []

    def send(ci, shard, to, first=False):
        n = counts[ci]
        counts[ci] += 1
        cp = pltpu.make_async_remote_copy(
            src_ref=mine(ci) if first else slot(ci, shard),
            dst_ref=slot(ci, shard),
            send_sem=send_sem.at[ci, n],
            recv_sem=recv_sem.at[ci, shard],
            device_id=to,
            device_id_type=MESH,
        )
        cp.start()
        pending.append(cp)

    def arrived(ci, shard):
        pltpu.make_async_remote_copy(
            src_ref=slot(ci, shard),
            dst_ref=slot(ci, shard),
            send_sem=send_sem.at[ci, 0],
            recv_sem=recv_sem.at[ci, shard],
            device_id=place.ident(c=1 - place.c),
            device_id_type=MESH,
        ).wait_recv()

    def near(order):
        nx, ny = {"x": 1 - place.x}, {"y": 1 - place.y}
        return (ny, nx) if order == 0 else (nx, ny)

    sib = place.ident(c=1 - place.c)
    zs = [lax.rem(place.z + o, 4) for o in (1, 2, 3)]
    for ci in range(len(chunks)):
        n1, n2 = near(chunks[ci][-1])
        for z in zs:
            send(ci, me, place.ident(z=z), True)
        send(ci, me, place.ident(**n1), True)
        send(ci, me, place.ident(**n2), True)
        send(ci, me, sib, True)
    for ci in range(len(chunks)):
        cp = pltpu.make_async_copy(mine(ci), slot(ci, me), own_sem.at[ci])
        cp.start()

    def from_n1(ci, z):
        n1, n2 = near(chunks[ci][-1])
        shard = place.index(z=z, **n1)
        arrived(ci, shard)
        send(ci, shard, place.ident(**n2))
        send(ci, shard, sib)

    def step2(ci):
        n1, n2 = near(chunks[ci][-1])
        from_n1(ci, place.z)
        for z in zs:
            shard = place.index(z=z)
            arrived(ci, shard)
            send(ci, shard, place.ident(**n1))
            send(ci, shard, place.ident(**n2))
            send(ci, shard, sib)

    def step3(ci):
        for z in zs:
            from_n1(ci, z)

    def step4(ci):
        n1, n2 = near(chunks[ci][-1])
        for far in ({}, n1):
            for z in [place.z] + zs:
                shard = place.index(z=z, **n2, **far)
                arrived(ci, shard)
                send(ci, shard, sib)

    pairs = [list(range(i, min(i + 2, len(chunks)))) for i in range(0, len(chunks), 2)]
    for t in range(len(pairs) + 2):
        for stage, fn in ((0, step2), (1, step3), (2, step4)):
            if 0 <= t - stage < len(pairs):
                for ci in pairs[t - stage]:
                    fn(ci)
    for ci in range(len(chunks)):
        for x in range(2):
            for y in range(2):
                for z in range(4):
                    arrived(ci, place.index(x=x, y=y, z=z, c=1 - place.c))
    for ci in range(len(chunks)):
        pltpu.make_async_copy(mine(ci), slot(ci, me), own_sem.at[ci]).wait()
    for cp in pending:
        cp.wait_send()


def gather(arrays, chunks, cid):
    n = len(arrays)

    def kernel(*refs):
        gather_kernel(chunks, refs[:n], refs[n : 2 * n], *refs[2 * n :])

    return pl.pallas_call(
        kernel,
        out_shape=[jax.ShapeDtypeStruct((32 * a.shape[0], a.shape[1]), a.dtype) for a in arrays],
        in_specs=[pl.BlockSpec(memory_space=pl.ANY)] * n,
        out_specs=[pl.BlockSpec(memory_space=pl.ANY)] * n,
        scratch_shapes=[
            pltpu.SemaphoreType.DMA((len(chunks), 31)),
            pltpu.SemaphoreType.DMA((len(chunks), 32)),
            pltpu.SemaphoreType.DMA((len(chunks),)),
        ],
        compiler_params=pltpu.CompilerParams(collective_id=cid, has_side_effects=True),
        name="gather",
    )(*arrays)


def scatter_kernel(chunks, nin, refs):
    n = len(chunks)
    ins = refs[:nin]
    outs = refs[nin : 2 * nin]
    rest = refs[2 * nin :]
    own, rc, r1, r2, rz = (rest[i * n : (i + 1) * n] for i in range(5))
    own_sem, cs, cr, s1, q1, s2, q2, sz, qz = rest[5 * n :]
    place = Place()
    greet(place)
    sib = place.ident(c=1 - place.c)

    def src(ci, shard):
        a, rows, r0, nr, c0, nc, order = chunks[ci]
        return ins[a].at[pl.ds(pl.multiple_of(shard * rows + r0, 8), nr), pl.ds(c0, nc)]

    def near(order):
        nx, ny = {"x": 1 - place.x}, {"y": 1 - place.y}
        return (nx, ny) if order == 0 else (ny, nx)

    def shard_at(ci, f1, f2, dz, **kw):
        n1, n2 = near(chunks[ci][-1])
        kw = dict(kw)
        if f1:
            kw.update(n1)
        if f2:
            kw.update(n2)
        return place.index(z=lax.rem(place.z + dz, 4), **kw)

    slots = [(f1, f2, dz) for f1 in (1, 0) for f2 in (1, 0) for dz in (1, 2, 3, 0)]

    def core_copy(ci, i):
        f1, f2, dz = slots[i]
        return pltpu.make_async_remote_copy(
            src_ref=src(ci, shard_at(ci, f1, f2, dz, c=1 - place.c)),
            dst_ref=rc[ci].at[i],
            send_sem=cs.at[ci, i],
            recv_sem=cr.at[ci, i],
            device_id=sib,
            device_id_type=MESH,
        )

    def own_copy(ci, i):
        f1, f2, dz = slots[i]
        return pltpu.make_async_copy(src(ci, shard_at(ci, f1, f2, dz)), own[ci].at[i], own_sem.at[ci, i])

    def n1_copy(ci, i):
        n1, n2 = near(chunks[ci][-1])
        return pltpu.make_async_remote_copy(
            src_ref=own[ci].at[i], dst_ref=r1[ci].at[i], send_sem=s1.at[ci, i], recv_sem=q1.at[ci, i],
            device_id=place.ident(**n1), device_id_type=MESH,
        )

    def n2_copy(ci, i):
        n1, n2 = near(chunks[ci][-1])
        return pltpu.make_async_remote_copy(
            src_ref=own[ci].at[8 + i], dst_ref=r2[ci].at[i], send_sem=s2.at[ci, i], recv_sem=q2.at[ci, i],
            device_id=place.ident(**n2), device_id_type=MESH,
        )

    def z_copy(ci, i):
        dz = slots[12 + i][2]
        return pltpu.make_async_remote_copy(
            src_ref=own[ci].at[12 + i], dst_ref=rz[ci].at[i], send_sem=sz.at[ci, i], recv_sem=qz.at[ci, i],
            device_id=place.ident(z=lax.rem(place.z + dz, 4)), device_id_type=MESH,
        )

    def add(ci, i, buf, j):
        own[ci][i] = (own[ci][i].astype(F32) + buf[ci][j].astype(F32)).astype(BF)

    for ci in range(n):
        for i in range(16):
            core_copy(ci, i).start()
        for i in range(16):
            own_copy(ci, i).start()

    def stage1(ci):
        for i in range(16):
            own_copy(ci, i).wait()
            core_copy(ci, i).wait_recv()
            add(ci, i, rc, i)
            if i < 8:
                n1_copy(ci, i).start()

    def stage2(ci):
        for i in range(8):
            n1_copy(ci, i).wait_recv()
            add(ci, 8 + i, r1, i)
            if i < 4:
                n2_copy(ci, i).start()

    def stage3(ci):
        for i in range(4):
            n2_copy(ci, i).wait_recv()
            add(ci, 12 + i, r2, i)
            if i < 3:
                z_copy(ci, i).start()

    def stage4(ci):
        a, rows, r0, nr, c0, nc, order = chunks[ci]
        total = own[ci][15].astype(F32)
        for i in range(3):
            z_copy(ci, i).wait_recv()
            total = total + rz[ci][i].astype(F32)
        outs[a][pl.ds(r0, nr), pl.ds(c0, nc)] = total

    pairs = [list(range(i, min(i + 2, n))) for i in range(0, n, 2)]
    for t in range(len(pairs) + 3):
        for stage, fn in ((0, stage1), (1, stage2), (2, stage3), (3, stage4)):
            if 0 <= t - stage < len(pairs):
                for ci in pairs[t - stage]:
                    fn(ci)
    for ci in range(n):
        for i in range(16):
            core_copy(ci, i).wait_send()
        for i in range(8):
            n1_copy(ci, i).wait_send()
        for i in range(4):
            n2_copy(ci, i).wait_send()
        for i in range(3):
            z_copy(ci, i).wait_send()


def scatter(arrays, chunks, cid):
    n = len(chunks)
    nin = len(arrays)

    def kernel(*refs):
        scatter_kernel(chunks, nin, refs)

    def bufs(count):
        return [pltpu.VMEM((count, c[3], c[5]), BF) for c in chunks]

    sem = lambda k: pltpu.SemaphoreType.DMA((n, k))
    return pl.pallas_call(
        kernel,
        out_shape=[jax.ShapeDtypeStruct((a.shape[0] // 32, a.shape[1]), F32) for a in arrays],
        in_specs=[pl.BlockSpec(memory_space=pl.ANY)] * nin,
        out_specs=[pl.BlockSpec(memory_space=pltpu.VMEM)] * nin,
        scratch_shapes=bufs(16) + bufs(16) + bufs(8) + bufs(4) + bufs(3)
        + [sem(16), sem(16), sem(16), sem(8), sem(8), sem(4), sem(4), sem(3), sem(3)],
        compiler_params=pltpu.CompilerParams(collective_id=cid, has_side_effects=True, vmem_limit_bytes=60 << 20),
        name="scatter",
    )(*arrays)


SLOT0 = (0, 4, 7, 9)
LN_ROWS = 64


def lanes(shape):
    return lax.broadcasted_iota(jnp.int32, shape, 1)


def row_loop(seq, body):
    @pl.loop(0, seq // LN_ROWS)
    def _(t):
        body(pl.ds(pl.multiple_of(t * LN_ROWS, LN_ROWS), LN_ROWS))


def spread_mats(dim):
    r = lax.broadcasted_iota(jnp.int32, (dim // 4, dim), 0)
    h = lax.broadcasted_iota(jnp.int32, (dim // 4, dim), 1)
    return [jnp.where(h == 4 * r + c, 1.0, 0.0).astype(BF) for c in range(4)]


def fwd_steps(r):
    seq, dim = r.x.shape
    hid = r.wi.shape[1] // WIDTHS
    vec = r.vec

    def small():
        sm = r.wp[:, 4 * dim :].astype(F32).T
        vec[0:16, :] = sm[0:16]
        mats = spread_mats(dim)
        part = dim // WIDTHS
        for j in range(WIDTHS):
            row = jnp.zeros((8, dim), F32)
            for c in range(4):
                lhs = jnp.broadcast_to(sm[8 + c : 9 + c, part * j : part * (j + 1)], (8, part)).astype(BF)
                row = row + dot(lhs, mats[c])
            vec[16 + j : 17 + j, :] = row[0:1]

    def qkv():
        for t, bias in ((0, 0), (1, None), (2, 1)):
            @pl.loop(0, dim // 256)
            def _(n):
                cols = pl.ds(pl.multiple_of(n * 256, 256), 256)
                acc = dot(r.x[...], r.wp[:, pl.ds(pl.multiple_of(t * dim + n * 256, 256), 256)])
                if bias is not None:
                    acc = acc + vec[bias : bias + 1, cols]
                r.qkv[t, :, cols] = acc.astype(BF)

    def attention():
        same = r.segc[...] == r.segr[...]

        @pl.loop(0, HEADS // 2)
        def _(i):
            cols = pl.ds(pl.multiple_of(i * 128, 128), 128)
            q, k, v = r.qkv[0, :, cols], r.qkv[1, :, cols], r.qkv[2, :, cols]
            low = lanes(q.shape) < DH
            zero = jnp.zeros_like(q)
            outs = []
            lse = r.lse[...]
            for half in range(2):
                qh = jnp.where(low if half == 0 else ~low, q, zero)
                s = jnp.where(same, dot_nt(qh, k) * SCORE_SCALE, MASKED)
                m = jnp.max(s, axis=-1, keepdims=True)
                e = jnp.exp(s - m)
                total = jnp.sum(e, axis=-1, keepdims=True)
                p = (e * (1.0 / total)).astype(BF)
                outs.append(dot(p, v))
                lse = jnp.where(lanes(lse.shape) == 2 * i + half, m + jnp.log(total), lse)
            r.lse[...] = lse
            r.att[:, cols] = jnp.where(low, outs[0], outs[1]).astype(BF)

    def norm1():
        feat = dim // WIDTHS
        for k in range(WIDTHS):
            lo = (feat * k // 128) * 128
            win = r.att[:, lo : lo + 256]
            at = lanes(win.shape) + lo
            win = jnp.where((at >= feat * k) & (at < feat * (k + 1)), win, jnp.zeros_like(win))
            add = dot(win, r.wp[lo : lo + 256, 3 * dim : 4 * dim])
            r.br[...] = add if k == 0 else r.br[...] + add

            def body(rows, k=k):
                h = r.x[rows, :].astype(F32) + r.br[rows, :] + vec[2:3, :]
                c = h - jnp.mean(h, axis=-1, keepdims=True)
                inv = lax.rsqrt(jnp.mean(c * c, axis=-1, keepdims=True) + EPSILON)
                sc = c * inv
                first = sc * vec[3:4, :] + vec[4:5, :]
                r.first[k, rows, :] = first
                r.low[k, rows, :] = first.astype(BF)
                r.sc[k, rows, :] = sc.astype(BF)
                r.inv[rows, k : k + 1] = inv

            row_loop(seq, body)

    def inner():
        @pl.loop(0, WIDTHS)
        def _(j):
            start = lax.div(j * (9 - j), 2)

            @pl.loop(0, hid // 256)
            def _(n):
                cols = pl.ds(pl.multiple_of(n * 256, 256), 256)
                wcols = pl.ds(pl.multiple_of(j * hid + n * 256, 256), 256)
                bias = vec[pl.ds(16 + j, 1), cols]

                @pl.loop(j, WIDTHS)
                def _(k):
                    pre = dot(r.low[k], r.wi[:, wcols]) + bias
                    phi = 0.5 * (1.0 + lax.erf(pre * 0.7071067811865476))
                    slope = phi + pre * (jnp.exp(-0.5 * pre * pre) * 0.3989422804014327)
                    r.act[start + k - j, :, cols] = (pre * phi).astype(BF)
                    r.slope[start + k - j, :, cols] = slope.astype(BF)

    def outer(k):
        def run():
            @pl.loop(0, dim // 256)
            def _(n):
                cols = pl.ds(pl.multiple_of(n * 256, 256), 256)
                acc = dot(r.act[SLOT0[0] + k], r.wu[0:hid, cols])
                for j in range(1, k + 1):
                    acc = acc + dot(r.act[SLOT0[j] + k - j], r.wu[hid * j : hid * (j + 1), cols])
                r.br[:, cols] = acc

            def body(rows):
                h = r.first[k, rows, :] + r.br[rows, :] + vec[5:6, :]
                c = h - jnp.mean(h, axis=-1, keepdims=True)
                inv = lax.rsqrt(jnp.mean(c * c, axis=-1, keepdims=True) + EPSILON)
                sc = c * inv
                r.out[k, rows, :] = (sc * vec[6:7, :] + vec[7:8, :]).astype(BF)
                up = r.up[k, rows, :].astype(F32)
                tg = up * vec[6:7, :]
                ts = tg * sc
                back = inv * (tg - jnp.mean(tg, axis=-1, keepdims=True) - sc * jnp.mean(ts, axis=-1, keepdims=True))
                ob = back.astype(BF)
                r.ob[k, rows, :] = ob
                r.acc[0:1, :] += jnp.sum(up * sc, axis=0, keepdims=True)
                r.acc[1:2, :] += jnp.sum(up, axis=0, keepdims=True)
                r.acc[2:3, :] += jnp.sum(ob.astype(F32), axis=0, keepdims=True)

            row_loop(seq, body)
        return run

    def clear():
        r.acc[...] = jnp.zeros_like(r.acc)
        r.lse[...] = jnp.zeros_like(r.lse)
        r.inv[...] = jnp.zeros_like(r.inv)

    return dict(clear=clear, small=small, qkv=qkv, attention=attention, norm1=norm1, inner=inner,
                outer=[outer(k) for k in range(WIDTHS)])


class Refs:
    pass


def named(names, refs):
    r = Refs()
    for name, ref in zip(names, refs):
        setattr(r, name, ref)
    return r


FWD_IN = ("x", "segc", "segr", "up", "hp", "hi", "hu")
FWD_OUT = ("hout", "hact", "hslope", "hlow", "hob", "hsc", "hqkv", "hatt", "inv", "lse", "vec", "acc")
FWD_SCRATCH = ("wp", "wi", "wu", "qkv", "att", "br", "first", "low", "act", "slope", "out", "ob", "sc", "sem")


def forward(x, segc, segr, up, hp, hi, hu):
    seq, dim = x.shape
    ff = hi.shape[1]
    hid = ff // WIDTHS
    row = (seq, dim)
    names = FWD_IN + FWD_OUT + FWD_SCRATCH

    def kernel(*refs):
        r = named(names, refs)
        s = fwd_steps(r)
        loads = [pltpu.make_async_copy(a, b, r.sem.at[i]) for i, (a, b) in
                 enumerate(((r.hp, r.wp), (r.hi, r.wi), (r.hu, r.wu)))]
        for cp in loads:
            cp.start()
        s["clear"]()
        loads[0].wait()
        s["small"]()
        s["qkv"]()
        s["attention"]()
        s["norm1"]()
        loads[1].wait()
        s["inner"]()
        stores = [pltpu.make_async_copy(a, b, r.sem.at[3 + i]) for i, (a, b) in enumerate(
            ((r.act, r.hact), (r.slope, r.hslope), (r.low, r.hlow), (r.sc, r.hsc), (r.qkv, r.hqkv), (r.att, r.hatt)))]
        for cp in stores:
            cp.start()
        loads[2].wait()
        for k in range(WIDTHS):
            s["outer"][k]()
        late = [pltpu.make_async_copy(r.out, r.hout, r.sem.at[9]), pltpu.make_async_copy(r.ob, r.hob, r.sem.at[10])]
        for cp in late:
            cp.start()
        for cp in stores + late:
            cp.wait()

    any_ = pl.BlockSpec(memory_space=pl.ANY)
    vm = pl.BlockSpec(memory_space=pltpu.VMEM)
    S = jax.ShapeDtypeStruct
    out_shape = [S((4,) + row, BF), S((10, seq, hid), BF), S((10, seq, hid), BF), S((4,) + row, BF), S((4,) + row, BF),
                 S((4,) + row, BF), S((3,) + row, BF), S(row, BF), S((seq, 128), F32), S((seq, 128), F32),
                 S((24, dim), F32), S((24, dim), F32)]
    V = pltpu.VMEM
    return pl.pallas_call(
        kernel,
        out_shape=out_shape,
        in_specs=[vm, vm, vm, vm, any_, any_, any_],
        out_specs=[any_] * 8 + [vm] * 4,
        scratch_shapes=[V(hp.shape, BF), V(hi.shape, BF), V(hu.shape, BF), V((3,) + row, BF), V(row, BF), V(row, F32),
                        V((4,) + row, F32), V((4,) + row, BF), V((10, seq, hid), BF), V((10, seq, hid), BF),
                        V((4,) + row, BF), V((4,) + row, BF), V((4,) + row, BF), pltpu.SemaphoreType.DMA((11,))],
        compiler_params=pltpu.CompilerParams(vmem_limit_bytes=64 * 1000 * 1000),
        name="forward",
    )(x, segc, segr, up, hp, hi, hu)


BWD_IN = ("x", "segc", "segr", "inv", "lse", "vec", "acc0", "hob", "hact", "hslope", "hlow", "hsc", "hu", "hi", "hp",
          "hqkv", "hatt")
BWD_OUT = ("xg", "gp", "gi", "gu")
BWD_SCRATCH = ("ob", "act", "slope", "low", "sc", "wu", "wi", "wp", "qkv", "att", "fb", "tot", "acc", "abi", "stage",
               "sem", "gsem")


def bwd_steps(r, emit):
    seq, dim = r.x.shape
    hid = r.wi.shape[1] // WIDTHS
    vec = r.vec
    feat = dim // WIDTHS
    half = dim // 2

    def d_outer(j):
        for m in range(hid // half):
            lhs = r.act[SLOT0[j] * seq : (SLOT0[j] + WIDTHS - j) * seq, m * half : (m + 1) * half]
            emit(2, dot_tn(lhs, r.ob[j * seq :, :]), hid * j + m * half, 0)

    def inner_back():
        @pl.loop(0, WIDTHS)
        def _(j):
            start = lax.div(j * (9 - j), 2)

            @pl.loop(0, hid // 256)
            def _(n):
                cols = pl.ds(pl.multiple_of(n * 256, 256), 256)
                wrows = pl.ds(pl.multiple_of(j * hid + n * 256, 256), 256)

                @pl.loop(j, WIDTHS)
                def _(k):
                    rows = pl.ds(pl.multiple_of((start + k - j) * seq, seq), seq)
                    grad = dot_nt(r.ob[pl.ds(pl.multiple_of(k * seq, seq), seq), :], r.wu[wrows, :])
                    ib = (grad * r.slope[rows, cols].astype(F32)).astype(BF)
                    r.slope[rows, cols] = ib
                    r.abi[pl.ds(j, 1), cols] += jnp.sum(ib.astype(F32), axis=0, keepdims=True)

    def d_inner(j):
        for m in range(dim // half):
            lhs = r.low[j * seq :, m * half : (m + 1) * half]
            emit(1, dot_tn(lhs, r.slope[SLOT0[j] * seq : (SLOT0[j] + WIDTHS - j) * seq, :]), m * half, hid * j)

    def first_back(k):
        def slot(j):
            at = (SLOT0[j] + k - j) * seq
            return r.slope[at : at + seq, :]

        @pl.loop(0, dim // 256)
        def _(n):
            cols = pl.ds(pl.multiple_of(n * 256, 256), 256)
            acc = r.ob[k * seq : (k + 1) * seq, cols].astype(F32)
            for j in range(k + 1):
                acc = acc + dot_nt(slot(j), r.wi[cols, hid * j : hid * (j + 1)])
            r.fb[:, cols] = acc

        def body(rows):
            fb = r.fb[rows, :]
            at = pl.ds(rows.start + k * seq, LN_ROWS)
            sc = r.sc[at, :].astype(F32)
            fs = fb * sc
            r.acc[3:4, :] += jnp.sum(fs, axis=0, keepdims=True)
            r.acc[4:5, :] += jnp.sum(fb, axis=0, keepdims=True)
            gain = vec[3:4, :]
            tg = fb * gain
            ab = r.inv[rows, k : k + 1] * (
                tg - jnp.mean(tg, axis=-1, keepdims=True) - sc * jnp.mean(fs * gain, axis=-1, keepdims=True))
            tot = ab if k == WIDTHS - 1 else r.tot[rows, :] + ab
            r.tot[rows, :] = tot
            r.act[pl.ds(rows.start + k * seq, LN_ROWS), :] = tot.astype(BF)
            if k == 0:
                r.acc[5:6, :] += jnp.sum(tot, axis=0, keepdims=True)

        row_loop(seq, body)

    def suffix(k):
        return r.act[k * seq : (k + 1) * seq, :]

    def d_output():
        for m in range(2):
            lhs = r.att[:, m * half : (m + 1) * half]
            one = dot_tn(lhs, suffix(2 * m))
            two = dot_tn(lhs, suffix(2 * m + 1))
            emit(0, jnp.concatenate([one[:feat], two[feat:]], axis=0), m * half, 3 * dim)

    def att_back():
        for m in range(2):
            w = r.wp[m * half : (m + 1) * half, 3 * dim : 4 * dim]
            one = dot_nt(suffix(2 * m), w)
            two = dot_nt(suffix(2 * m + 1), w)
            r.act[4 * seq : 5 * seq, m * half : (m + 1) * half] = jnp.where(
                lanes(one.shape) < feat, one, two).astype(BF)

    def attention_back():
        same = r.segc[...] == r.segr[...]

        @pl.loop(0, HEADS // 2)
        def _(i):
            cols = pl.ds(pl.multiple_of(i * 128, 128), 128)
            q, k, v = r.qkv[0, :, cols], r.qkv[1, :, cols], r.qkv[2, :, cols]
            g = r.act[4 * seq : 5 * seq, cols]
            low = lanes(q.shape) < DH
            zero = jnp.zeros_like(q)
            lse = r.lse[...]
            res = []
            for hf in range(2):
                mine = low if hf == 0 else ~low
                qh = jnp.where(mine, q, zero)
                gh = jnp.where(mine, g, zero)
                s = jnp.where(same, dot_nt(qh, k) * SCORE_SCALE, MASKED)
                col = jnp.sum(jnp.where(lanes(lse.shape) == 2 * i + hf, lse, 0.0), axis=-1, keepdims=True)
                p = jnp.exp(s - col)
                dp = dot_nt(gh, v)
                ds = (p * (dp - jnp.sum(p * dp, axis=-1, keepdims=True))).astype(BF)
                res.append((dot(ds, k), dot_tn(ds, q), dot_tn(p.astype(BF), g)))
            for t, scale in ((0, SCORE_SCALE), (1, SCORE_SCALE), (2, 1.0)):
                r.act[(5 + t) * seq : (6 + t) * seq, cols] = (
                    jnp.where(low, res[0][t], res[1][t]) * scale).astype(BF)

    def d_qkv(t):
        grad = r.act[(5 + t) * seq : (6 + t) * seq, :]
        for m in range(2):
            emit(0, dot_tn(r.x[:, m * half : (m + 1) * half], grad), m * half, t * dim)
        if t != 1:
            r.acc[6 + t // 2 : 7 + t // 2, :] = jnp.sum(grad.astype(F32), axis=0, keepdims=True)

    def input_grad():
        @pl.loop(0, dim // 256)
        def _(n):
            cols = pl.ds(pl.multiple_of(n * 256, 256), 256)
            acc = r.tot[:, cols]
            for t in range(3):
                acc = acc + dot_nt(r.act[(5 + t) * seq : (6 + t) * seq, :], r.wp[cols, t * dim : (t + 1) * dim])
            r.xg[:, cols] = acc

    def small():
        mats = spread_mats(dim)
        part = dim // WIDTHS
        bi = r.abi[...].astype(BF)
        rows = []
        for c in range(4):
            moved = [dot_nt(bi, mats[c])[j : j + 1] for j in range(WIDTHS)]
            rows.append(jnp.concatenate(moved, axis=1))
        a = r.acc
        vecs = [a[6:7, :], a[7:8, :], a[5:6, :], a[3:4, :], a[4:5, :], a[2:3, :], a[0:1, :], a[1:2, :]]
        tall = jnp.concatenate(vecs + rows + [jnp.zeros((128 - 12, dim), F32)], axis=0)
        return tall.T.astype(BF)

    def clear():
        r.acc[0:3, :] = r.acc0[0:3, :]
        r.acc[3:24, :] = jnp.zeros((21, dim), F32)
        r.abi[...] = jnp.zeros_like(r.abi)

    return dict(clear=clear, d_outer=d_outer, inner_back=inner_back, d_inner=d_inner, first_back=first_back,
                d_output=d_output, att_back=att_back, attention_back=attention_back, d_qkv=d_qkv,
                input_grad=input_grad, small=small)


def backward(x, segc, segr, saved, hu, hi, hp):
    hout, hact, hslope, hlow, hob, hsc, hqkv, hatt, inv, lse, vec, acc0 = saved
    seq, dim = x.shape
    ff = hi.shape[1]
    hid = ff // WIDTHS
    names = BWD_IN + BWD_OUT + BWD_SCRATCH

    def kernel(*refs):
        r = named(names, refs)
        order = [(r.hob, r.ob), (r.hact, r.act), (r.hu, r.wu), (r.hslope, r.slope), (r.hlow, r.low), (r.hi, r.wi),
                 (r.hsc, r.sc), (r.hatt, r.att), (r.hp, r.wp), (r.hqkv, r.qkv)]
        loads = [pltpu.make_async_copy(a, b, r.sem.at[i]) for i, (a, b) in enumerate(order)]
        for cp in loads:
            cp.start()
        outs = (r.gp, r.gi, r.gu)
        flying = [None, None]
        turn = [0]

        def emit(a, value, row, col):
            t = turn[0] % 2
            turn[0] += 1
            if flying[t] is not None:
                flying[t].wait()
            rows, cols = value.shape
            r.stage[t, :, :] = value.astype(BF)
            cp = pltpu.make_async_copy(r.stage.at[t], outs[a].at[pl.ds(row, rows), pl.ds(col, cols)], r.gsem.at[t])
            cp.start()
            flying[t] = cp

        s = bwd_steps(r, emit)
        s["clear"]()
        loads[0].wait()
        loads[1].wait()
        for j in range(WIDTHS):
            s["d_outer"](j)
        loads[2].wait()
        loads[3].wait()
        s["inner_back"]()
        loads[4].wait()
        for j in range(WIDTHS):
            s["d_inner"](j)
        loads[5].wait()
        loads[6].wait()
        for k in range(WIDTHS - 1, -1, -1):
            s["first_back"](k)
        loads[7].wait()
        s["d_output"]()
        loads[8].wait()
        s["att_back"]()
        loads[9].wait()
        s["attention_back"]()
        for t in range(3):
            s["d_qkv"](t)
        s["input_grad"]()
        for cp in flying:
            cp.wait()
        r.stage[0, :, 0:128] = s["small"]()[: dim // 2]
        r.stage[1, :, 0:128] = s["small"]()[dim // 2 :]
        last = [pltpu.make_async_copy(r.stage.at[t, :, pl.ds(0, 128)],
                                      r.gp.at[pl.ds(t * (dim // 2), dim // 2), pl.ds(4 * dim, 128)], r.gsem.at[t])
                for t in range(2)]
        for cp in last:
            cp.start()
        for cp in last:
            cp.wait()

    any_ = pl.BlockSpec(memory_space=pl.ANY)
    vm = pl.BlockSpec(memory_space=pltpu.VMEM)
    S = jax.ShapeDtypeStruct
    V = pltpu.VMEM
    flat = lambda a: a.reshape(-1, a.shape[-1])
    return pl.pallas_call(
        kernel,
        out_shape=[S((seq, dim), F32), S(hp.shape, BF), S(hi.shape, BF), S(hu.shape, BF)],
        in_specs=[vm] * 7 + [any_] * 10,
        out_specs=[vm, any_, any_, any_],
        scratch_shapes=[V((4 * seq, dim), BF), V((10 * seq, hid), BF), V((10 * seq, hid), BF), V((4 * seq, dim), BF),
                        V((4 * seq, dim), BF), V(hu.shape, BF), V(hi.shape, BF), V(hp.shape, BF),
                        V((3, seq, dim), BF), V((seq, dim), BF), V((seq, dim), F32), V((seq, dim), F32),
                        V((24, dim), F32), V((8, dim), F32), V((2, dim // 2, dim), BF),
                        pltpu.SemaphoreType.DMA((10,)), pltpu.SemaphoreType.DMA((2,))],
        compiler_params=pltpu.CompilerParams(vmem_limit_bytes=64 * 1000 * 1000),
        name="backward",
    )(x, segc, segr, inv, lse, vec, acc0, flat(hob), flat(hact), flat(hslope), flat(hlow), flat(hsc), hu, hi, hp,
      hqkv, hatt)


def direct(rows):
    return lax.axis_size("dp") == 2 and lax.axis_size("fsdp") == 16 and rows % 8 == 0


def per_device(inputs, segments, out_grads, wq, bq, wk, wv, bv, wo, bo, g1, s1, wi, bi, wu, bu, g2, s2):
    rows = wq.shape[0]
    dim = wq.shape[1]
    ff = wi.shape[1]
    feat = dim // WIDTHS
    hid = ff // WIDTHS
    small = jnp.concatenate(
        [jnp.stack([bq, bv, bo, g1, s1, bu, g2, s2], axis=1), bi.reshape(rows, ff // dim)], axis=1
    )
    nsmall = small.shape[1]
    small = jnp.pad(small, ((0, 0), (0, EXTRA - nsmall)))
    packed = jnp.concatenate([wq, wk, wv, wo, small], axis=1)
    width = packed.shape[1]
    own = direct(rows)
    if own:
        h = 13 * 128
        chunks = [
            (0, rows, 0, rows, 0, h, 0), (0, rows, 0, rows, h, width - h, 1),
            (1, rows, 0, rows, 0, ff // 2, 0), (1, rows, 0, rows, ff // 2, ff // 2, 1),
            (2, 4 * rows, 0, 2 * rows, 0, dim, 0), (2, 4 * rows, 2 * rows, 2 * rows, 0, dim, 1),
        ]
        full, wi_f, wu_f = gather([packed, wi, wu], chunks, 1)
    else:
        full, wi_f, wu_f = [lax.all_gather(a, AXES, axis=0, tiled=True) for a in (packed, wi, wu)]
    x = inputs[0]
    seg = segments[0]
    segc, segr = seg[:, None], seg[None, :]
    saved = forward(x, segc, segr, out_grads[:, 0], full, wi_f, wu_f)
    x_grad, d_packed, d_wi, d_wu = backward(x, segc, segr, saved, wu_f, wi_f, full)
    if own:
        order = chunks[2:] + chunks[:2]
        red, r_wi, r_wu = scatter([d_packed, d_wi, d_wu], order, 2)
    else:
        red, r_wi, r_wu = [
            lax.psum_scatter(a, AXES, scatter_dimension=0, tiled=True).astype(F32) for a in (d_packed, d_wi, d_wu)
        ]
    rs = red[:, 4 * dim :]
    vecs = [rs[:, i] for i in range(8)]
    r_bi = rs[:, 8 : 8 + ff // dim].reshape(-1)
    return (
        saved[0][:, None],
        x_grad[None],
        red[:, :dim],
        vecs[0],
        red[:, dim : 2 * dim],
        red[:, 2 * dim : 3 * dim],
        vecs[1],
        red[:, 3 * dim : 4 * dim],
        vecs[2],
        vecs[3],
        vecs[4],
        r_wi,
        r_bi,
        r_wu,
        vecs[5],
        vecs[6],
        vecs[7],
    )


def solution(mesh):
    mat = P(AXES, None)
    vec = P(AXES)
    params = (mat, vec, mat, mat, vec, mat, vec, vec, vec, mat, vec, mat, vec, vec, vec)
    return jax.shard_map(
        per_device,
        mesh=mesh,
        in_specs=(P(AXES, None, None), P(AXES, None), P(None, AXES, None, None)) + params,
        out_specs=(P(None, AXES, None, None), P(AXES, None, None)) + params,
        check_vma=False,
    )
```

```python
import functools

import jax
import jax.numpy as jnp
from jax import lax
from jax.experimental import pallas as pl
from jax.experimental.pallas import tpu as pltpu
from jax.sharding import PartitionSpec as P

HEADS = 12
DH = 64
WIDTHS = 4
EPSILON = 1e-12
SCORE_SCALE = 0.125
MASKED = -1000000000.0
BF = jnp.bfloat16
F32 = jnp.float32
AXES = ("dp", "fsdp")
EXTRA = 128


def dot(a, b):
    return jnp.dot(a, b, preferred_element_type=F32)


def dot_tn(a, b):
    return lax.dot_general(a, b, (((0,), (0,)), ((), ())), preferred_element_type=F32)


def dot_nt(a, b):
    return lax.dot_general(a, b, (((1,), (1,)), ((), ())), preferred_element_type=F32)


MESH = pl.DeviceIdType.MESH
HALF = 384
SMALL = 2304
OUT = SMALL + EXTRA


class Place:
    def __init__(self):
        self.x = lax.axis_index("dp")
        f = lax.axis_index("fsdp")
        self.z = f // 4
        self.y = (f // 2) % 2
        self.c = f % 2

    def ident(self, x=None, z=None, y=None, c=None):
        x = self.x if x is None else x
        z = self.z if z is None else z
        y = self.y if y is None else y
        c = self.c if c is None else c
        return {"dp": x, "fsdp": z * 4 + y * 2 + c}

    def index(self, x=None, z=None, y=None, c=None):
        x = self.x if x is None else x
        z = self.z if z is None else z
        y = self.y if y is None else y
        c = self.c if c is None else c
        return x * 16 + z * 4 + y * 2 + c


def greet(place):
    barrier = pltpu.get_barrier_semaphore()
    others = [place.ident(z=lax.rem(place.z + o, 4)) for o in (1, 2, 3)]
    others += [place.ident(x=1 - place.x), place.ident(y=1 - place.y), place.ident(c=1 - place.c)]
    for other in others:
        pl.semaphore_signal(barrier, inc=1, device_id=other, device_id_type=MESH)
    pl.semaphore_wait(barrier, len(others))


def chunk_list(parts, order_first):
    return parts


def gather_kernel(chunks, ins, outs, send_sem, recv_sem, own_sem):
    place = Place()
    greet(place)
    me = place.index()
    counts = [0] * len(chunks)

    def mine(ci):
        a, rows, r0, nr, c0, nc, order = chunks[ci]
        return ins[a].at[pl.ds(r0, nr), pl.ds(c0, nc)]

    def slot(ci, shard):
        a, rows, r0, nr, c0, nc, order = chunks[ci]
        return outs[a].at[pl.ds(pl.multiple_of(shard * rows + r0, 8), nr), pl.ds(c0, nc)]

    pending = []

    def send(ci, shard, to, first=False):
        n = counts[ci]
        counts[ci] += 1
        cp = pltpu.make_async_remote_copy(
            src_ref=mine(ci) if first else slot(ci, shard),
            dst_ref=slot(ci, shard),
            send_sem=send_sem.at[ci, n],
            recv_sem=recv_sem.at[ci, shard],
            device_id=to,
            device_id_type=MESH,
        )
        cp.start()
        pending.append(cp)

    def arrived(ci, shard):
        pltpu.make_async_remote_copy(
            src_ref=slot(ci, shard),
            dst_ref=slot(ci, shard),
            send_sem=send_sem.at[ci, 0],
            recv_sem=recv_sem.at[ci, shard],
            device_id=place.ident(c=1 - place.c),
            device_id_type=MESH,
        ).wait_recv()

    def near(order):
        nx, ny = {"x": 1 - place.x}, {"y": 1 - place.y}
        return (ny, nx) if order == 0 else (nx, ny)

    sib = place.ident(c=1 - place.c)
    zs = [lax.rem(place.z + o, 4) for o in (1, 2, 3)]
    for ci in range(len(chunks)):
        n1, n2 = near(chunks[ci][-1])
        for z in zs:
            send(ci, me, place.ident(z=z), True)
        send(ci, me, place.ident(**n1), True)
        send(ci, me, place.ident(**n2), True)
        send(ci, me, sib, True)
    for ci in range(len(chunks)):
        cp = pltpu.make_async_copy(mine(ci), slot(ci, me), own_sem.at[ci])
        cp.start()

    def from_n1(ci, z):
        n1, n2 = near(chunks[ci][-1])
        shard = place.index(z=z, **n1)
        arrived(ci, shard)
        send(ci, shard, place.ident(**n2))
        send(ci, shard, sib)

    def step2(ci):
        n1, n2 = near(chunks[ci][-1])
        from_n1(ci, place.z)
        for z in zs:
            shard = place.index(z=z)
            arrived(ci, shard)
            send(ci, shard, place.ident(**n1))
            send(ci, shard, place.ident(**n2))
            send(ci, shard, sib)

    def step3(ci):
        for z in zs:
            from_n1(ci, z)

    def step4(ci):
        n1, n2 = near(chunks[ci][-1])
        for far in ({}, n1):
            for z in [place.z] + zs:
                shard = place.index(z=z, **n2, **far)
                arrived(ci, shard)
                send(ci, shard, sib)

    pairs = [list(range(i, min(i + 2, len(chunks)))) for i in range(0, len(chunks), 2)]
    for t in range(len(pairs) + 2):
        for stage, fn in ((0, step2), (1, step3), (2, step4)):
            if 0 <= t - stage < len(pairs):
                for ci in pairs[t - stage]:
                    fn(ci)
    for ci in range(len(chunks)):
        for x in range(2):
            for y in range(2):
                for z in range(4):
                    arrived(ci, place.index(x=x, y=y, z=z, c=1 - place.c))
    for ci in range(len(chunks)):
        pltpu.make_async_copy(mine(ci), slot(ci, me), own_sem.at[ci]).wait()
    for cp in pending:
        cp.wait_send()


def gather(arrays, chunks, cid):
    n = len(arrays)

    def kernel(*refs):
        gather_kernel(chunks, refs[:n], refs[n : 2 * n], *refs[2 * n :])

    return pl.pallas_call(
        kernel,
        out_shape=[jax.ShapeDtypeStruct((32 * a.shape[0], a.shape[1]), a.dtype) for a in arrays],
        in_specs=[pl.BlockSpec(memory_space=pl.ANY)] * n,
        out_specs=[pl.BlockSpec(memory_space=pl.ANY)] * n,
        scratch_shapes=[
            pltpu.SemaphoreType.DMA((len(chunks), 31)),
            pltpu.SemaphoreType.DMA((len(chunks), 32)),
            pltpu.SemaphoreType.DMA((len(chunks),)),
        ],
        compiler_params=pltpu.CompilerParams(collective_id=cid, has_side_effects=True),
        name="gather",
    )(*arrays)


SLOT0 = (0, 4, 7, 9)
LN_ROWS = 64


def lanes(shape):
    return lax.broadcasted_iota(jnp.int32, shape, 1)


def row_loop(seq, body):
    @pl.loop(0, seq // LN_ROWS)
    def _(t):
        body(pl.ds(pl.multiple_of(t * LN_ROWS, LN_ROWS), LN_ROWS))


def spread_mats(dim):
    r = lax.broadcasted_iota(jnp.int32, (dim // 4, dim), 0)
    h = lax.broadcasted_iota(jnp.int32, (dim // 4, dim), 1)
    return [jnp.where(h == 4 * r + c, 1.0, 0.0).astype(BF) for c in range(4)]


def fwd_steps(r):
    seq, dim = r.x.shape
    hid = r.wi.shape[1] // WIDTHS
    vec = r.vec

    def small():
        sm = r.wp[:, SMALL:OUT].astype(F32).T
        vec[0:16, :] = sm[0:16]
        mats = spread_mats(dim)
        part = dim // WIDTHS
        for j in range(WIDTHS):
            row = jnp.zeros((8, dim), F32)
            for c in range(4):
                lhs = jnp.broadcast_to(sm[8 + c : 9 + c, part * j : part * (j + 1)], (8, part)).astype(BF)
                row = row + dot(lhs, mats[c])
            vec[16 + j : 17 + j, :] = row[0:1]

    def qkv():
        for t, bias in ((0, 0), (1, None), (2, 1)):
            for h in range(2):
                at = 3 * HALF * h + HALF * t
                acc = dot(r.x[...], r.wp[:, at : at + HALF])
                if bias is not None:
                    acc = acc + vec[bias : bias + 1, HALF * h : HALF * (h + 1)]
                r.qkv[t, :, HALF * h : HALF * (h + 1)] = acc.astype(BF)

    def attention():
        same = r.segc[...] == r.segr[...]

        @pl.loop(0, HEADS // 2)
        def _(i):
            cols = pl.ds(pl.multiple_of(i * 128, 128), 128)
            q, k, v = r.qkv[0, :, cols], r.qkv[1, :, cols], r.qkv[2, :, cols]
            low = lanes(q.shape) < DH
            zero = jnp.zeros_like(q)
            outs = []
            lse = r.lse[...]
            for half in range(2):
                qh = jnp.where(low if half == 0 else ~low, q, zero)
                s = jnp.where(same, dot_nt(qh, k) * SCORE_SCALE, MASKED)
                m = jnp.max(s, axis=-1, keepdims=True)
                e = jnp.exp(s - m)
                total = jnp.sum(e, axis=-1, keepdims=True)
                p = (e * (1.0 / total)).astype(BF)
                outs.append(dot(p, v))
                lse = jnp.where(lanes(lse.shape) == 2 * i + half, m + jnp.log(total), lse)
            r.lse[...] = lse
            r.att[:, cols] = jnp.where(low, outs[0], outs[1]).astype(BF)

    def norm1():
        feat = dim // WIDTHS
        for k in range(WIDTHS):
            lo = (feat * k // 128) * 128
            win = r.att[:, lo : lo + 256]
            at = lanes(win.shape) + lo
            win = jnp.where((at >= feat * k) & (at < feat * (k + 1)), win, jnp.zeros_like(win))
            add = dot(win, r.wp[lo : lo + 256, OUT : OUT + dim])
            r.br[...] = add if k == 0 else r.br[...] + add

            def body(rows, k=k):
                h = r.x[rows, :].astype(F32) + r.br[rows, :] + vec[2:3, :]
                c = h - jnp.mean(h, axis=-1, keepdims=True)
                inv = lax.rsqrt(jnp.mean(c * c, axis=-1, keepdims=True) + EPSILON)
                sc = c * inv
                first = sc * vec[3:4, :] + vec[4:5, :]
                r.first[k, rows, :] = first
                r.low[k, rows, :] = first.astype(BF)
                r.sc[k, rows, :] = sc.astype(BF)
                r.inv[rows, k : k + 1] = inv

            row_loop(seq, body)

    def inner():
        @pl.loop(0, WIDTHS)
        def _(j):
            start = lax.div(j * (9 - j), 2)

            @pl.loop(0, hid // 256)
            def _(n):
                cols = pl.ds(pl.multiple_of(n * 256, 256), 256)
                wcols = pl.ds(pl.multiple_of(j * hid + n * 256, 256), 256)
                bias = vec[pl.ds(16 + j, 1), cols]

                @pl.loop(j, WIDTHS)
                def _(k):
                    pre = dot(r.low[k], r.wi[:, wcols]) + bias
                    phi = 0.5 * (1.0 + lax.erf(pre * 0.7071067811865476))
                    slope = phi + pre * (jnp.exp(-0.5 * pre * pre) * 0.3989422804014327)
                    r.act[start + k - j, :, cols] = (pre * phi).astype(BF)
                    r.slope[start + k - j, :, cols] = slope.astype(BF)

    def outer(k):
        def run():
            @pl.loop(0, dim // 256)
            def _(n):
                cols = pl.ds(pl.multiple_of(n * 256, 256), 256)
                acc = dot(r.act[SLOT0[0] + k], r.wu[0:hid, cols])
                for j in range(1, k + 1):
                    acc = acc + dot(r.act[SLOT0[j] + k - j], r.wu[hid * j : hid * (j + 1), cols])
                r.br[:, cols] = acc

            def body(rows):
                h = r.first[k, rows, :] + r.br[rows, :] + vec[5:6, :]
                c = h - jnp.mean(h, axis=-1, keepdims=True)
                inv = lax.rsqrt(jnp.mean(c * c, axis=-1, keepdims=True) + EPSILON)
                sc = c * inv
                r.out[k, rows, :] = (sc * vec[6:7, :] + vec[7:8, :]).astype(BF)
                up = r.up[k, rows, :].astype(F32)
                tg = up * vec[6:7, :]
                ts = tg * sc
                back = inv * (tg - jnp.mean(tg, axis=-1, keepdims=True) - sc * jnp.mean(ts, axis=-1, keepdims=True))
                ob = back.astype(BF)
                r.ob[k, rows, :] = ob
                r.acc[0:1, :] += jnp.sum(up * sc, axis=0, keepdims=True)
                r.acc[1:2, :] += jnp.sum(up, axis=0, keepdims=True)
                r.acc[2:3, :] += jnp.sum(ob.astype(F32), axis=0, keepdims=True)

            row_loop(seq, body)
        return run

    def clear():
        r.acc[...] = jnp.zeros_like(r.acc)
        r.lse[...] = jnp.zeros_like(r.lse)
        r.inv[...] = jnp.zeros_like(r.inv)

    return dict(clear=clear, small=small, qkv=qkv, attention=attention, norm1=norm1, inner=inner,
                outer=[outer(k) for k in range(WIDTHS)])


class Refs:
    pass


def named(names, refs):
    r = Refs()
    for name, ref in zip(names, refs):
        setattr(r, name, ref)
    return r


FWD_IN = ("x", "segc", "segr", "up", "hp", "hi", "hu")
FWD_OUT = ("hout", "hact", "hslope", "hlow", "hob", "hsc", "hqkv", "hatt", "inv", "lse", "vec", "acc")
FWD_SCRATCH = ("wp", "wi", "wu", "qkv", "att", "br", "first", "low", "act", "slope", "out", "ob", "sc", "sem")


def forward(x, segc, segr, up, hp, hi, hu):
    seq, dim = x.shape
    ff = hi.shape[1]
    hid = ff // WIDTHS
    row = (seq, dim)
    names = FWD_IN + FWD_OUT + FWD_SCRATCH

    def kernel(*refs):
        r = named(names, refs)
        s = fwd_steps(r)
        loads = [pltpu.make_async_copy(a, b, r.sem.at[i]) for i, (a, b) in
                 enumerate(((r.hp, r.wp), (r.hi, r.wi), (r.hu, r.wu)))]
        for cp in loads:
            cp.start()
        s["clear"]()
        loads[0].wait()
        s["small"]()
        s["qkv"]()
        s["attention"]()
        s["norm1"]()
        loads[1].wait()
        s["inner"]()
        stores = [pltpu.make_async_copy(a, b, r.sem.at[3 + i]) for i, (a, b) in enumerate(
            ((r.act, r.hact), (r.slope, r.hslope), (r.low, r.hlow), (r.sc, r.hsc), (r.qkv, r.hqkv), (r.att, r.hatt)))]
        for cp in stores:
            cp.start()
        loads[2].wait()
        for k in range(WIDTHS):
            s["outer"][k]()
        late = [pltpu.make_async_copy(r.out, r.hout, r.sem.at[9]), pltpu.make_async_copy(r.ob, r.hob, r.sem.at[10])]
        for cp in late:
            cp.start()
        for cp in stores + late:
            cp.wait()

    any_ = pl.BlockSpec(memory_space=pl.ANY)
    vm = pl.BlockSpec(memory_space=pltpu.VMEM)
    S = jax.ShapeDtypeStruct
    out_shape = [S((4,) + row, BF), S((10, seq, hid), BF), S((10, seq, hid), BF), S((4,) + row, BF), S((4,) + row, BF),
                 S((4,) + row, BF), S((3,) + row, BF), S(row, BF), S((seq, 128), F32), S((seq, 128), F32),
                 S((24, dim), F32), S((24, dim), F32)]
    V = pltpu.VMEM
    return pl.pallas_call(
        kernel,
        out_shape=out_shape,
        in_specs=[vm, vm, vm, vm, any_, any_, any_],
        out_specs=[any_] * 8 + [vm] * 4,
        scratch_shapes=[V(hp.shape, BF), V(hi.shape, BF), V(hu.shape, BF), V((3,) + row, BF), V(row, BF), V(row, F32),
                        V((4,) + row, F32), V((4,) + row, BF), V((10, seq, hid), BF), V((10, seq, hid), BF),
                        V((4,) + row, BF), V((4,) + row, BF), V((4,) + row, BF), pltpu.SemaphoreType.DMA((11,))],
        compiler_params=pltpu.CompilerParams(vmem_limit_bytes=64 * 1000 * 1000),
        name="forward",
    )(x, segc, segr, up, hp, hi, hu)


class Scatter:
    def __init__(self, chunks, src, bufs, sems):
        self.chunks = chunks
        self.src = src
        n = len(chunks)
        self.own, self.rc, self.r1, self.r2, self.rz = (bufs[i * n : (i + 1) * n] for i in range(5))
        self.sems = sems
        self.place = Place()

    def flips(self, ci, i):
        f1, f2, dz = 1 - i // 8, 1 - (i // 4) % 2, lax.rem(i + 1, 4)
        p = self.place
        fx, fy = (f1, f2) if self.chunks[ci][-1] == 0 else (f2, f1)
        return dict(x=lax.rem(p.x + fx, 2), y=lax.rem(p.y + fy, 2), z=lax.rem(p.z + dz, 4))

    def near(self, ci):
        nx, ny = {"x": 1 - self.place.x}, {"y": 1 - self.place.y}
        return (nx, ny) if self.chunks[ci][-1] == 0 else (ny, nx)

    def rows(self, ci, shard):
        a, rows, r0, nr, c0, nc, order = self.chunks[ci]
        return self.src[a].at[pl.ds(pl.multiple_of(shard * rows + r0, 8), nr), pl.ds(c0, nc)]

    def remote(self, ci, src, dst, send, recv, i, to):
        return pltpu.make_async_remote_copy(
            src_ref=src, dst_ref=dst, send_sem=self.sems[send].at[ci, i], recv_sem=self.sems[recv].at[ci, i],
            device_id=to, device_id_type=MESH,
        )

    def core(self, ci, i):
        p = self.place
        shard = p.index(c=1 - p.c, **self.flips(ci, i))
        return self.remote(ci, self.rows(ci, shard), self.rc[ci].at[i], 1, 2, i, p.ident(c=1 - p.c))

    def load(self, ci, i):
        shard = self.place.index(**self.flips(ci, i))
        return pltpu.make_async_copy(self.rows(ci, shard), self.own[ci].at[i], self.sems[0].at[ci, i])

    def first(self, ci, i):
        to = self.place.ident(**self.near(ci)[0])
        return self.remote(ci, self.own[ci].at[i], self.r1[ci].at[i], 3, 4, i, to)

    def second(self, ci, i):
        to = self.place.ident(**self.near(ci)[1])
        return self.remote(ci, self.own[ci].at[8 + i], self.r2[ci].at[i], 5, 6, i, to)

    def along(self, ci, i):
        to = self.place.ident(z=lax.rem(self.place.z + i + 1, 4))
        return self.remote(ci, self.own[ci].at[12 + i], self.rz[ci].at[i], 7, 8, i, to)

    def add(self, ci, i, buf, j):
        self.own[ci][i] = (self.own[ci][i].astype(F32) + buf[ci][j].astype(F32)).astype(BF)

    def start(self, ci):
        @pl.loop(0, 16)
        def _(i):
            self.core(ci, i).start()
            self.load(ci, i).start()

    def stage1(self, ci):
        @pl.loop(0, 16)
        def _(i):
            self.load(ci, i).wait()
            self.core(ci, i).wait_recv()
            self.add(ci, i, self.rc, i)

            @pl.when(i < 8)
            def _():
                self.first(ci, i).start()

    def stage2(self, ci):
        @pl.loop(0, 8)
        def _(i):
            self.first(ci, i).wait_recv()
            self.add(ci, 8 + i, self.r1, i)

            @pl.when(i < 4)
            def _():
                self.second(ci, i).start()

    def stage3(self, ci):
        @pl.loop(0, 4)
        def _(i):
            self.second(ci, i).wait_recv()
            self.add(ci, 12 + i, self.r2, i)

            @pl.when(i < 3)
            def _():
                self.along(ci, i).start()

    def stage4(self, ci):
        total = self.own[ci][15].astype(F32)
        for i in range(3):
            self.along(ci, i).wait_recv()
            total = total + self.rz[ci][i].astype(F32)
        return total

    def finish(self, ci):
        for count, fn in ((16, self.core), (8, self.first), (4, self.second), (3, self.along)):
            @pl.loop(0, count)
            def _(i):
                fn(ci, i).wait_send()


def scatter_chunks(rows, dim, ff):
    u = [(2, 4 * rows, h * 2 * rows, 2 * rows, 0, dim, h) for h in range(2)]
    i = [(1, rows, 0, rows, h * ff // 2, ff // 2, h) for h in range(2)]
    o = [(0, rows, 0, rows, OUT + HALF * h, HALF, h) for h in range(2)]
    q0 = [(0, rows, 0, rows, 0, 640, 0), (0, rows, 0, rows, 640, 512, 1)]
    q1 = [(0, rows, 0, rows, 1152, 640, 0), (0, rows, 0, rows, 1792, 640, 1)]
    return u + i + o + q0 + q1


BWD_IN = ("x", "segc", "segr", "inv", "lse", "vec", "acc0", "hob", "hact", "hslope", "hlow", "hsc", "hu", "hi", "hp",
          "hqkv", "hatt")
BWD_OUT = ("xg", "gp", "gi", "gu")
BWD_SCRATCH = ("ob", "act", "slope", "low", "w", "tot", "acc", "abi", "stage", "sem", "gsem")


def bwd_steps(r, emit):
    seq, dim = r.x.shape
    hid = r.slope.shape[1]
    vec = r.vec
    feat = dim // WIDTHS
    half = dim // 2

    def d_outer(j):
        for m in range(hid // half):
            lhs = r.act[SLOT0[j] * seq : (SLOT0[j] + WIDTHS - j) * seq, m * half : (m + 1) * half]
            emit(2, dot_tn(lhs, r.ob[j * seq :, :]), hid * j + m * half, 0)

    def inner_back(first, last):
        @pl.loop(first, last)
        def _(j):
            start = lax.div(j * (9 - j), 2)

            @pl.loop(0, hid // 256)
            def _(n):
                cols = pl.ds(pl.multiple_of(n * 256, 256), 256)
                wrows = pl.ds(pl.multiple_of(j * hid + n * 256, 256), 256)

                @pl.loop(j, WIDTHS)
                def _(k):
                    rows = pl.ds(pl.multiple_of((start + k - j) * seq, seq), seq)
                    grad = dot_nt(r.ob[pl.ds(pl.multiple_of(k * seq, seq), seq), :], r.w[wrows, :])
                    ib = (grad * r.slope[rows, cols].astype(F32)).astype(BF)
                    r.slope[rows, cols] = ib
                    r.abi[pl.ds(j, 1), cols] += jnp.sum(ib.astype(F32), axis=0, keepdims=True)

    def d_inner(j):
        for m in range(dim // half):
            lhs = r.low[j * seq :, m * half : (m + 1) * half]
            emit(1, dot_tn(lhs, r.slope[SLOT0[j] * seq : (SLOT0[j] + WIDTHS - j) * seq, :]), m * half, hid * j)

    def first_back(k):
        def slot(j):
            at = (SLOT0[j] + k - j) * seq
            return r.slope[at : at + seq, :]

        @pl.loop(0, dim // 256)
        def _(n):
            cols = pl.ds(pl.multiple_of(n * 256, 256), 256)
            acc = r.ob[k * seq : (k + 1) * seq, cols].astype(F32)
            for j in range(k + 1):
                acc = acc + dot_nt(slot(j), r.w[pl.ds(pl.multiple_of(n * 256 + dim * j, 256), 256), :])
            r.xg[:, cols] = acc

        def body(rows):
            fb = r.xg[rows, :]
            at = pl.ds(rows.start + k * seq, LN_ROWS)
            sc = r.act[at, :].astype(F32)
            fs = fb * sc
            r.acc[3:4, :] += jnp.sum(fs, axis=0, keepdims=True)
            r.acc[4:5, :] += jnp.sum(fb, axis=0, keepdims=True)
            gain = vec[3:4, :]
            tg = fb * gain
            ab = r.inv[rows, k : k + 1] * (
                tg - jnp.mean(tg, axis=-1, keepdims=True) - sc * jnp.mean(fs * gain, axis=-1, keepdims=True))
            tot = ab if k == WIDTHS - 1 else r.tot[rows, :] + ab
            r.tot[rows, :] = tot
            r.act[pl.ds(rows.start + k * seq, LN_ROWS), :] = tot.astype(BF)
            if k == 0:
                r.acc[5:6, :] += jnp.sum(tot, axis=0, keepdims=True)

        row_loop(seq, body)

    def suffix(k):
        return r.act[k * seq : (k + 1) * seq, :]

    def d_output():
        for m in range(2):
            lhs = r.low[3 * seq :, m * half : (m + 1) * half]
            one = dot_tn(lhs, suffix(2 * m))
            two = dot_tn(lhs, suffix(2 * m + 1))
            emit(0, jnp.concatenate([one[:feat], two[feat:]], axis=0), m * half, OUT)

    def att_back():
        for m in range(2):
            w = r.w[3 * dim + m * half : 3 * dim + (m + 1) * half, :]
            one = dot_nt(suffix(2 * m), w)
            two = dot_nt(suffix(2 * m + 1), w)
            r.act[4 * seq : 5 * seq, m * half : (m + 1) * half] = jnp.where(
                lanes(one.shape) < feat, one, two).astype(BF)

    def attention_back(first, last):
        same = r.segc[...] == r.segr[...]

        @pl.loop(first, last)
        def _(i):
            cols = pl.ds(pl.multiple_of(i * 128, 128), 128)
            q, k, v = r.low[0:seq, cols], r.low[seq : 2 * seq, cols], r.low[2 * seq : 3 * seq, cols]
            g = r.act[4 * seq : 5 * seq, cols]
            low = lanes(q.shape) < DH
            zero = jnp.zeros_like(q)
            lse = r.lse[...]
            res = []
            for hf in range(2):
                mine = low if hf == 0 else ~low
                qh = jnp.where(mine, q, zero)
                gh = jnp.where(mine, g, zero)
                s = jnp.where(same, dot_nt(qh, k) * SCORE_SCALE, MASKED)
                col = jnp.sum(jnp.where(lanes(lse.shape) == 2 * i + hf, lse, 0.0), axis=-1, keepdims=True)
                p = jnp.exp(s - col)
                dp = dot_nt(gh, v)
                ds = (p * (dp - jnp.sum(p * dp, axis=-1, keepdims=True))).astype(BF)
                res.append((dot(ds, k), dot_tn(ds, q), dot_tn(p.astype(BF), g)))
            for t, scale in ((0, SCORE_SCALE), (1, SCORE_SCALE), (2, 1.0)):
                r.act[(5 + t) * seq : (6 + t) * seq, cols] = (
                    jnp.where(low, res[0][t], res[1][t]) * scale).astype(BF)

    def d_qkv(h):
        for t in range(3):
            cols = slice(HALF * h, HALF * (h + 1))
            grad = r.act[(5 + t) * seq : (6 + t) * seq, cols]
            for m in range(2):
                emit(0, dot_tn(r.x[:, m * half : (m + 1) * half], grad), m * half, 3 * HALF * h + HALF * t)
            if t != 1:
                r.acc[6 + t // 2 : 7 + t // 2, cols] = jnp.sum(grad.astype(F32), axis=0, keepdims=True)

    def input_grad():
        @pl.loop(0, dim // 256)
        def _(n):
            cols = pl.ds(pl.multiple_of(n * 256, 256), 256)
            acc = r.tot[:, cols]
            for t in range(3):
                acc = acc + dot_nt(r.act[(5 + t) * seq : (6 + t) * seq, :],
                                   r.w[pl.ds(pl.multiple_of(n * 256 + dim * t, 256), 256), :])
            r.xg[:, cols] = acc

    def small():
        mats = spread_mats(dim)
        part = dim // WIDTHS
        bi = r.abi[...].astype(BF)
        rows = []
        for c in range(4):
            moved = [dot_nt(bi, mats[c])[j : j + 1] for j in range(WIDTHS)]
            rows.append(jnp.concatenate(moved, axis=1))
        a = r.acc
        vecs = [a[6:7, :], a[7:8, :], a[5:6, :], a[3:4, :], a[4:5, :], a[2:3, :], a[0:1, :], a[1:2, :]]
        tall = jnp.concatenate(vecs + rows + [jnp.zeros((128 - 12, dim), F32)], axis=0)
        flipped = tall.T
        for m in range(2):
            emit(0, flipped[m * half : (m + 1) * half], m * half, SMALL)

    def clear():
        r.acc[0:3, :] = r.acc0[0:3, :]
        r.acc[3:24, :] = jnp.zeros((21, dim), F32)
        r.abi[...] = jnp.zeros_like(r.abi)

    return dict(clear=clear, d_outer=d_outer, inner_back=inner_back, d_inner=d_inner, first_back=first_back,
                d_output=d_output, att_back=att_back, attention_back=attention_back, d_qkv=d_qkv,
                input_grad=input_grad, small=small)


def backward(x, segc, segr, saved, hu, hi, hp, own):
    hout, hact, hslope, hlow, hob, hsc, hqkv, hatt, inv, lse, vec, acc0 = saved
    seq, dim = x.shape
    ff = hi.shape[1]
    hid = ff // WIDTHS
    rows = dim // 32
    chunks = scatter_chunks(rows, dim, ff) if own else []
    nc = len(chunks)
    extra = ("oq", "ok", "ov", "oo", "oi", "ou", "os") if own else ()
    names = BWD_IN + BWD_OUT + extra + BWD_SCRATCH

    def kernel(*refs):
        r = named(names, refs)
        if own:
            base = len(names)
            sc = Scatter(chunks, (r.gp, r.gi, r.gu), refs[base : base + 5 * nc], refs[base + 5 * nc : -1])
            packed = refs[-1]
            greet(sc.place)
        nsem = [0]

        def load(pairs):
            cps = []
            for a, b in pairs:
                cps.append(pltpu.make_async_copy(a, b, r.sem.at[nsem[0]]))
                nsem[0] += 1
                cps[-1].start()
            return cps

        def wait(cps):
            for cp in cps:
                cp.wait()

        l_ob = load([(r.hob, r.ob), (r.hact, r.act)])
        l_u = load([(r.hu, r.w), (r.hslope, r.slope)])
        l_low = load([(r.hlow, r.low)])
        outs = (r.gp, r.gi, r.gu)
        flying = [None, None]
        turn = [0]

        def emit(a, value, row, col):
            t = turn[0] % 2
            turn[0] += 1
            if flying[t] is not None:
                flying[t].wait()
            nr, ncol = value.shape
            r.stage[t, :, 0:ncol] = value.astype(BF)
            cp = pltpu.make_async_copy(r.stage.at[t, :, pl.ds(0, ncol)],
                                       outs[a].at[pl.ds(row, nr), pl.ds(col, ncol)], r.gsem.at[t])
            cp.start()
            flying[t] = cp

        def flush():
            for t in range(2):
                if flying[t] is not None:
                    flying[t].wait()
                    flying[t] = None

        U, I, O, Q0, Q1 = ((2 * g, 2 * g + 1) for g in range(5))

        def go(group):
            flush()
            if own:
                for ci in group:
                    sc.start(ci)

        def st(n, group):
            if own:
                for ci in group:
                    if n < 4:
                        (sc.stage1, sc.stage2, sc.stage3)[n - 1](ci)
                    else:
                        a, _, r0, nr, c0, ncol, _ = chunks[ci]
                        (packed, r.oi, r.ou)[a][r0 : r0 + nr, c0 : c0 + ncol] = sc.stage4(ci)

        s = bwd_steps(r, emit)
        s["clear"]()
        wait(l_ob)
        for j in range(WIDTHS):
            s["d_outer"](j)
        go(U)
        l_sc = load([(r.hsc, r.act.at[pl.ds(0, 4 * seq), :])])
        wait(l_u)
        s["inner_back"](0, 1)
        st(1, U)
        s["inner_back"](1, WIDTHS)
        l_i = load([(r.hi.at[:, pl.ds(hid * j, hid)], r.w.at[pl.ds(dim * j, dim), :]) for j in range(WIDTHS)])
        st(2, U)
        wait(l_low)
        s["d_inner"](0)
        s["d_inner"](1)
        st(3, U)
        s["d_inner"](2)
        s["d_inner"](3)
        go(I)
        l_q = load([(r.hqkv, r.low.at[pl.ds(0, 3 * seq), :]), (r.hatt, r.low.at[pl.ds(3 * seq, seq), :])])
        st(4, U)
        wait(l_sc)
        wait(l_i)
        s["first_back"](3)
        st(1, I)
        s["first_back"](2)
        st(2, I)
        s["first_back"](1)
        s["first_back"](0)
        l_p = load([(r.hp.at[:, pl.ds(OUT, dim)], r.w.at[pl.ds(3 * dim, dim), :])])
        l_p2 = load([(r.hp.at[:, pl.ds(3 * HALF * h + HALF * t, HALF)],
                      r.w.at[pl.ds(dim * t, dim), pl.ds(HALF * h, HALF)]) for t in range(3) for h in range(2)])
        st(3, I)
        wait(l_q)
        s["d_output"]()
        wait(l_p)
        s["att_back"]()
        go(O)
        st(4, I)
        s["attention_back"](0, 3)
        st(1, O)
        s["d_qkv"](0)
        go(Q0)
        st(2, O)
        s["attention_back"](3, 6)
        st(1, Q0)
        st(3, O)
        s["d_qkv"](1)
        s["small"]()
        go(Q1)
        st(2, Q0)
        st(4, O)
        wait(l_p2)
        s["input_grad"]()
        st(1, Q1)
        st(3, Q0)
        st(2, Q1)
        st(4, Q0)
        st(3, Q1)
        st(4, Q1)
        if own:
            for t, ref in enumerate((r.oq, r.ok, r.ov)):
                for h in range(2):
                    at = 3 * HALF * h + HALF * t
                    ref[:, HALF * h : HALF * (h + 1)] = packed[:, at : at + HALF]
            r.oo[...] = packed[:, OUT : OUT + dim]
            r.os[...] = packed[:, SMALL:OUT]
            for ci in range(nc):
                sc.finish(ci)

    any_ = pl.BlockSpec(memory_space=pl.ANY)
    vm = pl.BlockSpec(memory_space=pltpu.VMEM)
    S = jax.ShapeDtypeStruct
    V = pltpu.VMEM
    flat = lambda a: a.reshape(-1, a.shape[-1])
    out_shape = [S((seq, dim), F32), S(hp.shape, BF), S(hi.shape, BF), S(hu.shape, BF)]
    scratch = [V((4 * seq, dim), BF), V((10 * seq, hid), BF), V((10 * seq, hid), BF), V((4 * seq, dim), BF),
               V((ff, dim), BF), V((seq, dim), F32), V((24, dim), F32), V((8, dim), F32),
               V((2, dim // 2, dim), BF), pltpu.SemaphoreType.DMA((24,)), pltpu.SemaphoreType.DMA((2,))]
    params = dict(vmem_limit_bytes=67043328)
    if own:
        out_shape += [S((rows, dim), F32)] * 4 + [S((rows, ff), F32), S((4 * rows, dim), F32), S((rows, EXTRA), F32)]
        for count in (16, 16, 8, 4, 3):
            scratch += [V((count, c[3], c[5]), BF) for c in chunks]
        scratch += [pltpu.SemaphoreType.DMA((nc, k)) for k in (16, 16, 16, 8, 8, 4, 4, 3, 3)]
        scratch += [V((rows, hp.shape[1]), F32)]
        params.update(collective_id=2, has_side_effects=True)
    return pl.pallas_call(
        kernel,
        out_shape=out_shape,
        in_specs=[vm] * 7 + [any_] * 10,
        out_specs=[vm, any_, any_, any_] + [vm] * len(extra),
        scratch_shapes=scratch,
        compiler_params=pltpu.CompilerParams(**params),
        name="backward",
    )(x, segc, segr, inv, lse, vec, acc0, flat(hob), flat(hact), flat(hslope), flat(hlow), flat(hsc), hu, hi, hp,
      flat(hqkv), hatt)


def direct(rows):
    return lax.axis_size("dp") == 2 and lax.axis_size("fsdp") == 16 and rows % 8 == 0


def per_device(inputs, segments, out_grads, wq, bq, wk, wv, bv, wo, bo, g1, s1, wi, bi, wu, bu, g2, s2):
    rows, dim = wq.shape
    ff = wi.shape[1]
    per = ff // dim
    small = jnp.stack([bq, bv, bo, g1, s1, bu, g2, s2], axis=1)
    small = jnp.concatenate([small, bi.reshape(rows, per), jnp.zeros((rows, EXTRA - 8 - per), BF)], axis=1)
    cut = [w[:, HALF * h : HALF * (h + 1)] for h in range(2) for w in (wq, wk, wv)]
    packed = jnp.concatenate(cut + [small, wo], axis=1)
    width = packed.shape[1]
    own = direct(rows)
    if own:
        h = 13 * 128
        chunks = [
            (0, rows, 0, rows, 0, h, 0), (0, rows, 0, rows, h, width - h, 1),
            (1, rows, 0, rows, 0, ff // 2, 0), (1, rows, 0, rows, ff // 2, ff // 2, 1),
            (2, 4 * rows, 0, 2 * rows, 0, dim, 0), (2, 4 * rows, 2 * rows, 2 * rows, 0, dim, 1),
        ]
        full, wi_f, wu_f = gather([packed, wi, wu], chunks, 1)
    else:
        full, wi_f, wu_f = [lax.all_gather(a, AXES, axis=0, tiled=True) for a in (packed, wi, wu)]
    x = inputs[0]
    seg = segments[0]
    segc, segr = seg[:, None], seg[None, :]
    saved = forward(x, segc, segr, out_grads[:, 0], full, wi_f, wu_f)
    done = backward(x, segc, segr, saved, wu_f, wi_f, full, own)
    x_grad = done[0]
    if own:
        gq, gk, gv, go, gi, gu, rs = done[4:]
    else:
        red, gi, gu = [lax.psum_scatter(a, AXES, scatter_dimension=0, tiled=True).astype(F32) for a in done[1:4]]
        gq, gk, gv = [
            jnp.concatenate([red[:, 3 * HALF * h + HALF * t :][:, :HALF] for h in range(2)], axis=1) for t in range(3)
        ]
        rs, go = red[:, SMALL:OUT], red[:, OUT:]
    vecs = [rs[:, i] for i in range(8)]
    gb = rs[:, 8 : 8 + per].reshape(-1)
    return (saved[0][:, None], x_grad[None], gq, vecs[0], gk, gv, vecs[1], go, vecs[2], vecs[3], vecs[4], gi, gb, gu,
            vecs[5], vecs[6], vecs[7])


def solution(mesh):
    mat = P(AXES, None)
    vec = P(AXES)
    params = (mat, vec, mat, mat, vec, mat, vec, vec, vec, mat, vec, mat, vec, vec, vec)
    return jax.shard_map(
        per_device,
        mesh=mesh,
        in_specs=(P(AXES, None, None), P(AXES, None), P(None, AXES, None, None)) + params,
        out_specs=(P(None, AXES, None, None), P(AXES, None, None)) + params,
        check_vma=False,
    )
```

```python
import functools

import jax
import jax.numpy as jnp
from jax import lax
from jax.experimental import pallas as pl
from jax.experimental.pallas import tpu as pltpu
from jax.sharding import PartitionSpec as P

HEADS = 12
DH = 64
WIDTHS = 4
EPSILON = 1e-12
SCORE_SCALE = 0.125
MASKED = -1000000000.0
BF = jnp.bfloat16
F32 = jnp.float32
AXES = ("dp", "fsdp")
EXTRA = 128


def dot(a, b):
    return jnp.dot(a, b, preferred_element_type=F32)


def dot_tn(a, b):
    return lax.dot_general(a, b, (((0,), (0,)), ((), ())), preferred_element_type=F32)


def dot_nt(a, b):
    return lax.dot_general(a, b, (((1,), (1,)), ((), ())), preferred_element_type=F32)


MESH = pl.DeviceIdType.MESH
HALF = 384
SMALL = 2304
OUT = SMALL + EXTRA


class Place:
    def __init__(self):
        self.x = lax.axis_index("dp")
        f = lax.axis_index("fsdp")
        self.z = f // 4
        self.y = (f // 2) % 2
        self.c = f % 2

    def ident(self, x=None, z=None, y=None, c=None):
        x = self.x if x is None else x
        z = self.z if z is None else z
        y = self.y if y is None else y
        c = self.c if c is None else c
        return {"dp": x, "fsdp": z * 4 + y * 2 + c}

    def index(self, x=None, z=None, y=None, c=None):
        x = self.x if x is None else x
        z = self.z if z is None else z
        y = self.y if y is None else y
        c = self.c if c is None else c
        return x * 16 + z * 4 + y * 2 + c


def greet(place):
    barrier = pltpu.get_barrier_semaphore()
    others = [place.ident(z=lax.rem(place.z + o, 4)) for o in (1, 2, 3)]
    others += [place.ident(x=1 - place.x), place.ident(y=1 - place.y), place.ident(c=1 - place.c)]
    for other in others:
        pl.semaphore_signal(barrier, inc=1, device_id=other, device_id_type=MESH)
    pl.semaphore_wait(barrier, len(others))


def chunk_list(parts, order_first):
    return parts


def gather_kernel(chunks, ins, outs, send_sem, recv_sem, own_sem):
    place = Place()
    greet(place)
    me = place.index()
    counts = [0] * len(chunks)

    def mine(ci):
        a, rows, r0, nr, c0, nc, order = chunks[ci]
        return ins[a].at[pl.ds(r0, nr), pl.ds(c0, nc)]

    def slot(ci, shard):
        a, rows, r0, nr, c0, nc, order = chunks[ci]
        return outs[a].at[pl.ds(pl.multiple_of(shard * rows + r0, 8), nr), pl.ds(c0, nc)]

    pending = []

    def send(ci, shard, to, first=False):
        n = counts[ci]
        counts[ci] += 1
        cp = pltpu.make_async_remote_copy(
            src_ref=mine(ci) if first else slot(ci, shard),
            dst_ref=slot(ci, shard),
            send_sem=send_sem.at[ci, n],
            recv_sem=recv_sem.at[ci, shard],
            device_id=to,
            device_id_type=MESH,
        )
        cp.start()
        pending.append(cp)

    def arrived(ci, shard):
        pltpu.make_async_remote_copy(
            src_ref=slot(ci, shard),
            dst_ref=slot(ci, shard),
            send_sem=send_sem.at[ci, 0],
            recv_sem=recv_sem.at[ci, shard],
            device_id=place.ident(c=1 - place.c),
            device_id_type=MESH,
        ).wait_recv()

    def near(order):
        nx, ny = {"x": 1 - place.x}, {"y": 1 - place.y}
        return (ny, nx) if order == 0 else (nx, ny)

    sib = place.ident(c=1 - place.c)
    zs = [lax.rem(place.z + o, 4) for o in (1, 2, 3)]
    for ci in range(len(chunks)):
        n1, n2 = near(chunks[ci][-1])
        for z in zs:
            send(ci, me, place.ident(z=z), True)
        send(ci, me, place.ident(**n1), True)
        send(ci, me, place.ident(**n2), True)
        send(ci, me, sib, True)
    for ci in range(len(chunks)):
        cp = pltpu.make_async_copy(mine(ci), slot(ci, me), own_sem.at[ci])
        cp.start()

    def from_n1(ci, z):
        n1, n2 = near(chunks[ci][-1])
        shard = place.index(z=z, **n1)
        arrived(ci, shard)
        send(ci, shard, place.ident(**n2))
        send(ci, shard, sib)

    def step2(ci):
        n1, n2 = near(chunks[ci][-1])
        from_n1(ci, place.z)
        for z in zs:
            shard = place.index(z=z)
            arrived(ci, shard)
            send(ci, shard, place.ident(**n1))
            send(ci, shard, place.ident(**n2))
            send(ci, shard, sib)

    def step3(ci):
        for z in zs:
            from_n1(ci, z)

    def step4(ci):
        n1, n2 = near(chunks[ci][-1])
        for far in ({}, n1):
            for z in [place.z] + zs:
                shard = place.index(z=z, **n2, **far)
                arrived(ci, shard)
                send(ci, shard, sib)

    pairs = [list(range(i, min(i + 2, len(chunks)))) for i in range(0, len(chunks), 2)]
    for t in range(len(pairs) + 2):
        for stage, fn in ((0, step2), (1, step3), (2, step4)):
            if 0 <= t - stage < len(pairs):
                for ci in pairs[t - stage]:
                    fn(ci)
    for ci in range(len(chunks)):
        for x in range(2):
            for y in range(2):
                for z in range(4):
                    arrived(ci, place.index(x=x, y=y, z=z, c=1 - place.c))
    for ci in range(len(chunks)):
        pltpu.make_async_copy(mine(ci), slot(ci, me), own_sem.at[ci]).wait()
    for cp in pending:
        cp.wait_send()


def gather(arrays, chunks, cid):
    n = len(arrays)

    def kernel(*refs):
        gather_kernel(chunks, refs[:n], refs[n : 2 * n], *refs[2 * n :])

    return pl.pallas_call(
        kernel,
        out_shape=[jax.ShapeDtypeStruct((32 * a.shape[0], a.shape[1]), a.dtype) for a in arrays],
        in_specs=[pl.BlockSpec(memory_space=pl.ANY)] * n,
        out_specs=[pl.BlockSpec(memory_space=pl.ANY)] * n,
        scratch_shapes=[
            pltpu.SemaphoreType.DMA((len(chunks), 31)),
            pltpu.SemaphoreType.DMA((len(chunks), 32)),
            pltpu.SemaphoreType.DMA((len(chunks),)),
        ],
        compiler_params=pltpu.CompilerParams(collective_id=cid, has_side_effects=True),
        name="gather",
    )(*arrays)


SLOT0 = (0, 4, 7, 9)
LN_ROWS = 64


def lanes(shape):
    return lax.broadcasted_iota(jnp.int32, shape, 1)


def row_loop(seq, body):
    @pl.loop(0, seq // LN_ROWS)
    def _(t):
        body(pl.ds(pl.multiple_of(t * LN_ROWS, LN_ROWS), LN_ROWS))


def spread_mats(dim):
    r = lax.broadcasted_iota(jnp.int32, (dim // 4, dim), 0)
    h = lax.broadcasted_iota(jnp.int32, (dim // 4, dim), 1)
    return [jnp.where(h == 4 * r + c, 1.0, 0.0).astype(BF) for c in range(4)]


def fwd_steps(r):
    seq, dim = r.x.shape
    hid = r.wi.shape[1] // WIDTHS
    vec = r.vec

    def small():
        sm = r.wp[:, SMALL:OUT].astype(F32).T
        vec[0:16, :] = sm[0:16]
        mats = spread_mats(dim)
        part = dim // WIDTHS
        for j in range(WIDTHS):
            row = jnp.zeros((8, dim), F32)
            for c in range(4):
                lhs = jnp.broadcast_to(sm[8 + c : 9 + c, part * j : part * (j + 1)], (8, part)).astype(BF)
                row = row + dot(lhs, mats[c])
            vec[16 + j : 17 + j, :] = row[0:1]

    def qkv():
        for t, bias in ((0, 0), (1, None), (2, 1)):
            for h in range(2):
                at = 3 * HALF * h + HALF * t
                acc = dot(r.x[...], r.wp[:, at : at + HALF])
                if bias is not None:
                    acc = acc + vec[bias : bias + 1, HALF * h : HALF * (h + 1)]
                r.qkv[t, :, HALF * h : HALF * (h + 1)] = acc.astype(BF)

    def attention():
        same = r.segc[...] == r.segr[...]

        @pl.loop(0, HEADS // 2)
        def _(i):
            cols = pl.ds(pl.multiple_of(i * 128, 128), 128)
            q, k, v = r.qkv[0, :, cols], r.qkv[1, :, cols], r.qkv[2, :, cols]
            low = lanes(q.shape) < DH
            zero = jnp.zeros_like(q)
            outs = []
            lse = r.lse[...]
            for half in range(2):
                qh = jnp.where(low if half == 0 else ~low, q, zero)
                s = jnp.where(same, dot_nt(qh, k) * SCORE_SCALE, MASKED)
                m = jnp.max(s, axis=-1, keepdims=True)
                e = jnp.exp(s - m)
                total = jnp.sum(e, axis=-1, keepdims=True)
                p = (e * (1.0 / total)).astype(BF)
                outs.append(dot(p, v))
                lse = jnp.where(lanes(lse.shape) == 2 * i + half, m + jnp.log(total), lse)
            r.lse[...] = lse
            r.att[:, cols] = jnp.where(low, outs[0], outs[1]).astype(BF)

    def norm1():
        feat = dim // WIDTHS
        for k in range(WIDTHS):
            lo = (feat * k // 128) * 128
            win = r.att[:, lo : lo + 256]
            at = lanes(win.shape) + lo
            win = jnp.where((at >= feat * k) & (at < feat * (k + 1)), win, jnp.zeros_like(win))
            add = dot(win, r.wp[lo : lo + 256, OUT : OUT + dim])
            r.br[...] = add if k == 0 else r.br[...] + add

            def body(rows, k=k):
                h = r.x[rows, :].astype(F32) + r.br[rows, :] + vec[2:3, :]
                c = h - jnp.mean(h, axis=-1, keepdims=True)
                inv = lax.rsqrt(jnp.mean(c * c, axis=-1, keepdims=True) + EPSILON)
                sc = c * inv
                first = sc * vec[3:4, :] + vec[4:5, :]
                r.first[k, rows, :] = first
                r.low[k, rows, :] = first.astype(BF)
                r.sc[k, rows, :] = sc.astype(BF)
                r.inv[rows, k : k + 1] = inv

            row_loop(seq, body)

    def inner():
        @pl.loop(0, WIDTHS)
        def _(j):
            start = lax.div(j * (9 - j), 2)

            @pl.loop(0, hid // 256)
            def _(n):
                cols = pl.ds(pl.multiple_of(n * 256, 256), 256)
                wcols = pl.ds(pl.multiple_of(j * hid + n * 256, 256), 256)
                bias = vec[pl.ds(16 + j, 1), cols]

                @pl.loop(j, WIDTHS)
                def _(k):
                    pre = dot(r.low[k], r.wi[:, wcols]) + bias
                    phi = 0.5 * (1.0 + lax.erf(pre * 0.7071067811865476))
                    slope = phi + pre * (jnp.exp(-0.5 * pre * pre) * 0.3989422804014327)
                    r.act[start + k - j, :, cols] = (pre * phi).astype(BF)
                    r.slope[start + k - j, :, cols] = slope.astype(BF)

    def outer(k):
        def run():
            @pl.loop(0, dim // 256)
            def _(n):
                cols = pl.ds(pl.multiple_of(n * 256, 256), 256)
                acc = dot(r.act[SLOT0[0] + k], r.wu[0:hid, cols])
                for j in range(1, k + 1):
                    acc = acc + dot(r.act[SLOT0[j] + k - j], r.wu[hid * j : hid * (j + 1), cols])
                r.br[:, cols] = acc

            def body(rows):
                h = r.first[k, rows, :] + r.br[rows, :] + vec[5:6, :]
                c = h - jnp.mean(h, axis=-1, keepdims=True)
                inv = lax.rsqrt(jnp.mean(c * c, axis=-1, keepdims=True) + EPSILON)
                sc = c * inv
                r.out[k, rows, :] = (sc * vec[6:7, :] + vec[7:8, :]).astype(BF)
                up = r.up[k, rows, :].astype(F32)
                tg = up * vec[6:7, :]
                ts = tg * sc
                back = inv * (tg - jnp.mean(tg, axis=-1, keepdims=True) - sc * jnp.mean(ts, axis=-1, keepdims=True))
                ob = back.astype(BF)
                r.ob[k, rows, :] = ob
                r.acc[0:1, :] += jnp.sum(up * sc, axis=0, keepdims=True)
                r.acc[1:2, :] += jnp.sum(up, axis=0, keepdims=True)
                r.acc[2:3, :] += jnp.sum(ob.astype(F32), axis=0, keepdims=True)

            row_loop(seq, body)
        return run

    def clear():
        r.acc[...] = jnp.zeros_like(r.acc)
        r.lse[...] = jnp.zeros_like(r.lse)
        r.inv[...] = jnp.zeros_like(r.inv)

    return dict(clear=clear, small=small, qkv=qkv, attention=attention, norm1=norm1, inner=inner,
                outer=[outer(k) for k in range(WIDTHS)])


class Refs:
    pass


def named(names, refs):
    r = Refs()
    for name, ref in zip(names, refs):
        setattr(r, name, ref)
    return r


FWD_IN = ("x", "segc", "segr", "up", "hp", "hi", "hu")
FWD_OUT = ("hout", "hact", "hslope", "hlow", "hob", "hsc", "hqkv", "hatt", "inv", "lse", "vec", "acc")
FWD_SCRATCH = ("wp", "wi", "wu", "qkv", "att", "br", "first", "low", "act", "slope", "out", "ob", "sc", "sem")


def forward(x, segc, segr, up, hp, hi, hu):
    seq, dim = x.shape
    ff = hi.shape[1]
    hid = ff // WIDTHS
    row = (seq, dim)
    names = FWD_IN + FWD_OUT + FWD_SCRATCH

    def kernel(*refs):
        r = named(names, refs)
        s = fwd_steps(r)
        loads = [pltpu.make_async_copy(a, b, r.sem.at[i]) for i, (a, b) in
                 enumerate(((r.hp, r.wp), (r.hi, r.wi), (r.hu, r.wu)))]
        for cp in loads:
            cp.start()
        s["clear"]()
        loads[0].wait()
        s["small"]()
        s["qkv"]()
        s["attention"]()
        s["norm1"]()
        loads[1].wait()
        s["inner"]()
        stores = [pltpu.make_async_copy(a, b, r.sem.at[3 + i]) for i, (a, b) in enumerate(
            ((r.act, r.hact), (r.slope, r.hslope), (r.low, r.hlow), (r.sc, r.hsc), (r.qkv, r.hqkv), (r.att, r.hatt)))]
        for cp in stores:
            cp.start()
        loads[2].wait()
        for k in range(WIDTHS):
            s["outer"][k]()
        late = [pltpu.make_async_copy(r.out, r.hout, r.sem.at[9]), pltpu.make_async_copy(r.ob, r.hob, r.sem.at[10])]
        for cp in late:
            cp.start()
        for cp in stores + late:
            cp.wait()

    any_ = pl.BlockSpec(memory_space=pl.ANY)
    vm = pl.BlockSpec(memory_space=pltpu.VMEM)
    S = jax.ShapeDtypeStruct
    out_shape = [S((4,) + row, BF), S((10, seq, hid), BF), S((10, seq, hid), BF), S((4,) + row, BF), S((4,) + row, BF),
                 S((4,) + row, BF), S((3,) + row, BF), S(row, BF), S((seq, 128), F32), S((seq, 128), F32),
                 S((24, dim), F32), S((24, dim), F32)]
    V = pltpu.VMEM
    return pl.pallas_call(
        kernel,
        out_shape=out_shape,
        in_specs=[vm, vm, vm, vm, any_, any_, any_],
        out_specs=[any_] * 8 + [vm] * 4,
        scratch_shapes=[V(hp.shape, BF), V(hi.shape, BF), V(hu.shape, BF), V((3,) + row, BF), V(row, BF), V(row, F32),
                        V((4,) + row, F32), V((4,) + row, BF), V((10, seq, hid), BF), V((10, seq, hid), BF),
                        V((4,) + row, BF), V((4,) + row, BF), V((4,) + row, BF), pltpu.SemaphoreType.DMA((11,))],
        compiler_params=pltpu.CompilerParams(vmem_limit_bytes=64 * 1000 * 1000),
        name="forward",
    )(x, segc, segr, up, hp, hi, hu)


class Scatter:
    def __init__(self, chunks, src, bufs, sems):
        self.chunks = chunks
        self.src = src
        n = len(chunks)
        self.own, self.rc, self.r1, self.r2, self.rz = (bufs[i * n : (i + 1) * n] for i in range(5))
        self.sems = sems
        self.place = Place()

    def flips(self, ci, i):
        f1, f2, dz = 1 - i // 8, 1 - (i // 4) % 2, lax.rem(i + 1, 4)
        p = self.place
        fx, fy = (f1, f2) if self.chunks[ci][-1] == 0 else (f2, f1)
        return dict(x=lax.rem(p.x + fx, 2), y=lax.rem(p.y + fy, 2), z=lax.rem(p.z + dz, 4))

    def near(self, ci):
        nx, ny = {"x": 1 - self.place.x}, {"y": 1 - self.place.y}
        return (nx, ny) if self.chunks[ci][-1] == 0 else (ny, nx)

    def rows(self, ci, shard):
        a, rows, r0, nr, c0, nc, order = self.chunks[ci]
        return self.src[a].at[pl.ds(pl.multiple_of(shard * rows + r0, 8), nr), pl.ds(c0, nc)]

    def remote(self, ci, src, dst, send, recv, i, to):
        return pltpu.make_async_remote_copy(
            src_ref=src, dst_ref=dst, send_sem=self.sems[send].at[ci, i], recv_sem=self.sems[recv].at[ci, i],
            device_id=to, device_id_type=MESH,
        )

    def core(self, ci, i):
        p = self.place
        shard = p.index(c=1 - p.c, **self.flips(ci, i))
        return self.remote(ci, self.rows(ci, shard), self.rc[ci].at[i], 1, 2, i, p.ident(c=1 - p.c))

    def load(self, ci, i):
        shard = self.place.index(**self.flips(ci, i))
        return pltpu.make_async_copy(self.rows(ci, shard), self.own[ci].at[i], self.sems[0].at[ci, i])

    def first(self, ci, i):
        to = self.place.ident(**self.near(ci)[0])
        return self.remote(ci, self.own[ci].at[i], self.r1[ci].at[i], 3, 4, i, to)

    def second(self, ci, i):
        to = self.place.ident(**self.near(ci)[1])
        return self.remote(ci, self.own[ci].at[8 + i], self.r2[ci].at[i], 5, 6, i, to)

    def along(self, ci, i):
        to = self.place.ident(z=lax.rem(self.place.z + i + 1, 4))
        return self.remote(ci, self.own[ci].at[12 + i], self.rz[ci].at[i], 7, 8, i, to)

    def add(self, ci, i, buf, j):
        self.own[ci][i] = (self.own[ci][i].astype(F32) + buf[ci][j].astype(F32)).astype(BF)

    def start(self, ci):
        @pl.loop(0, 16)
        def _(i):
            self.core(ci, i).start()
            self.load(ci, i).start()

    def stage1(self, ci):
        @pl.loop(0, 16)
        def _(i):
            self.load(ci, i).wait()
            self.core(ci, i).wait_recv()
            self.add(ci, i, self.rc, i)

            @pl.when(i < 8)
            def _():
                self.first(ci, i).start()

    def stage2(self, ci):
        @pl.loop(0, 8)
        def _(i):
            self.first(ci, i).wait_recv()
            self.add(ci, 8 + i, self.r1, i)

            @pl.when(i < 4)
            def _():
                self.second(ci, i).start()

    def stage3(self, ci):
        @pl.loop(0, 4)
        def _(i):
            self.second(ci, i).wait_recv()
            self.add(ci, 12 + i, self.r2, i)

            @pl.when(i < 3)
            def _():
                self.along(ci, i).start()

    def stage4(self, ci):
        total = self.own[ci][15].astype(F32)
        for i in range(3):
            self.along(ci, i).wait_recv()
            total = total + self.rz[ci][i].astype(F32)
        return total

    def finish(self, ci):
        for count, fn in ((16, self.core), (8, self.first), (4, self.second), (3, self.along)):
            @pl.loop(0, count)
            def _(i):
                fn(ci, i).wait_send()


def scatter_chunks(rows, dim, ff):
    u = [(2, 4 * rows, h * 2 * rows, 2 * rows, 0, dim, h) for h in range(2)]
    i = [(1, rows, 0, rows, h * ff // 2, ff // 2, h) for h in range(2)]
    o = [(0, rows, 0, rows, OUT + HALF * h, HALF, h) for h in range(2)]
    q0 = [(0, rows, 0, rows, 0, 640, 0), (0, rows, 0, rows, 640, 512, 1)]
    q1 = [(0, rows, 0, rows, 1152, 640, 0), (0, rows, 0, rows, 1792, 640, 1)]
    return u + i + o + q0 + q1


BWD_IN = ("x", "segc", "segr", "inv", "lse", "vec", "acc0", "hob", "hact", "hslope", "hlow", "hsc", "hu", "hi", "hp",
          "hqkv", "hatt")
BWD_OUT = ("xg", "gp", "gi", "gu")
BWD_SCRATCH = ("ob", "act", "slope", "low", "w", "tot", "acc", "abi", "stage", "sem", "gsem")


def bwd_steps(r, emit):
    seq, dim = r.x.shape
    hid = r.slope.shape[1]
    vec = r.vec
    feat = dim // WIDTHS
    half = dim // 2

    def d_outer(j):
        for m in range(hid // half):
            lhs = r.act[SLOT0[j] * seq : (SLOT0[j] + WIDTHS - j) * seq, m * half : (m + 1) * half]
            emit(2, dot_tn(lhs, r.ob[j * seq :, :]), hid * j + m * half, 0)

    def inner_back(first, last):
        @pl.loop(first, last)
        def _(j):
            start = lax.div(j * (9 - j), 2)

            @pl.loop(0, hid // 256)
            def _(n):
                cols = pl.ds(pl.multiple_of(n * 256, 256), 256)
                wrows = pl.ds(pl.multiple_of(j * hid + n * 256, 256), 256)

                @pl.loop(j, WIDTHS)
                def _(k):
                    rows = pl.ds(pl.multiple_of((start + k - j) * seq, seq), seq)
                    grad = dot_nt(r.ob[pl.ds(pl.multiple_of(k * seq, seq), seq), :], r.w[wrows, :])
                    ib = (grad * r.slope[rows, cols].astype(F32)).astype(BF)
                    r.slope[rows, cols] = ib
                    r.abi[pl.ds(j, 1), cols] += jnp.sum(ib.astype(F32), axis=0, keepdims=True)

    def d_inner(j):
        for m in range(dim // half):
            lhs = r.low[j * seq :, m * half : (m + 1) * half]
            emit(1, dot_tn(lhs, r.slope[SLOT0[j] * seq : (SLOT0[j] + WIDTHS - j) * seq, :]), m * half, hid * j)

    def first_back(k):
        def slot(j):
            at = (SLOT0[j] + k - j) * seq
            return r.slope[at : at + seq, :]

        @pl.loop(0, dim // 256)
        def _(n):
            cols = pl.ds(pl.multiple_of(n * 256, 256), 256)
            acc = r.ob[k * seq : (k + 1) * seq, cols].astype(F32)
            for j in range(k + 1):
                acc = acc + dot_nt(slot(j), r.w[pl.ds(pl.multiple_of(n * 256 + dim * j, 256), 256), :])
            r.xg[:, cols] = acc

        def body(rows):
            fb = r.xg[rows, :]
            at = pl.ds(rows.start + k * seq, LN_ROWS)
            sc = r.act[at, :].astype(F32)
            fs = fb * sc
            r.acc[3:4, :] += jnp.sum(fs, axis=0, keepdims=True)
            r.acc[4:5, :] += jnp.sum(fb, axis=0, keepdims=True)
            gain = vec[3:4, :]
            tg = fb * gain
            ab = r.inv[rows, k : k + 1] * (
                tg - jnp.mean(tg, axis=-1, keepdims=True) - sc * jnp.mean(fs * gain, axis=-1, keepdims=True))
            tot = ab if k == WIDTHS - 1 else r.tot[rows, :] + ab
            r.tot[rows, :] = tot
            r.act[pl.ds(rows.start + k * seq, LN_ROWS), :] = tot.astype(BF)
            if k == 0:
                r.acc[5:6, :] += jnp.sum(tot, axis=0, keepdims=True)

        row_loop(seq, body)

    def suffix(k):
        return r.act[k * seq : (k + 1) * seq, :]

    def d_output():
        for m in range(2):
            lhs = r.low[3 * seq :, m * half : (m + 1) * half]
            one = dot_tn(lhs, suffix(2 * m))
            two = dot_tn(lhs, suffix(2 * m + 1))
            emit(0, jnp.concatenate([one[:feat], two[feat:]], axis=0), m * half, OUT)

    def att_back():
        for m in range(2):
            w = r.w[3 * dim + m * half : 3 * dim + (m + 1) * half, :]
            one = dot_nt(suffix(2 * m), w)
            two = dot_nt(suffix(2 * m + 1), w)
            r.act[4 * seq : 5 * seq, m * half : (m + 1) * half] = jnp.where(
                lanes(one.shape) < feat, one, two).astype(BF)

    def attention_back(first, last):
        same = r.segc[...] == r.segr[...]

        @pl.loop(first, last)
        def _(i):
            cols = pl.ds(pl.multiple_of(i * 128, 128), 128)
            q, k, v = r.low[0:seq, cols], r.low[seq : 2 * seq, cols], r.low[2 * seq : 3 * seq, cols]
            g = r.act[4 * seq : 5 * seq, cols]
            low = lanes(q.shape) < DH
            zero = jnp.zeros_like(q)
            lse = r.lse[...]
            res = []
            for hf in range(2):
                mine = low if hf == 0 else ~low
                qh = jnp.where(mine, q, zero)
                gh = jnp.where(mine, g, zero)
                s = jnp.where(same, dot_nt(qh, k) * SCORE_SCALE, MASKED)
                col = jnp.sum(jnp.where(lanes(lse.shape) == 2 * i + hf, lse, 0.0), axis=-1, keepdims=True)
                p = jnp.exp(s - col)
                dp = dot_nt(gh, v)
                ds = (p * (dp - jnp.sum(p * dp, axis=-1, keepdims=True))).astype(BF)
                res.append((dot(ds, k), dot_tn(ds, q), dot_tn(p.astype(BF), g)))
            for t, scale in ((0, SCORE_SCALE), (1, SCORE_SCALE), (2, 1.0)):
                r.act[(5 + t) * seq : (6 + t) * seq, cols] = (
                    jnp.where(low, res[0][t], res[1][t]) * scale).astype(BF)

    def d_qkv(h):
        for t in range(3):
            cols = slice(HALF * h, HALF * (h + 1))
            grad = r.act[(5 + t) * seq : (6 + t) * seq, cols]
            for m in range(2):
                emit(0, dot_tn(r.x[:, m * half : (m + 1) * half], grad), m * half, 3 * HALF * h + HALF * t)
            if t != 1:
                r.acc[6 + t // 2 : 7 + t // 2, cols] = jnp.sum(grad.astype(F32), axis=0, keepdims=True)

    def input_grad():
        @pl.loop(0, dim // 256)
        def _(n):
            cols = pl.ds(pl.multiple_of(n * 256, 256), 256)
            acc = r.tot[:, cols]
            for t in range(3):
                acc = acc + dot_nt(r.act[(5 + t) * seq : (6 + t) * seq, :],
                                   r.w[pl.ds(pl.multiple_of(n * 256 + dim * t, 256), 256), :])
            r.xg[:, cols] = acc

    def small():
        mats = spread_mats(dim)
        part = dim // WIDTHS
        bi = r.abi[...].astype(BF)
        rows = []
        for c in range(4):
            moved = [dot_nt(bi, mats[c])[j : j + 1] for j in range(WIDTHS)]
            rows.append(jnp.concatenate(moved, axis=1))
        a = r.acc
        vecs = [a[6:7, :], a[7:8, :], a[5:6, :], a[3:4, :], a[4:5, :], a[2:3, :], a[0:1, :], a[1:2, :]]
        tall = jnp.concatenate(vecs + rows + [jnp.zeros((128 - 12, dim), F32)], axis=0)
        flipped = tall.T
        for m in range(2):
            emit(0, flipped[m * half : (m + 1) * half], m * half, SMALL)

    def clear():
        r.acc[0:3, :] = r.acc0[0:3, :]
        r.acc[3:24, :] = jnp.zeros((21, dim), F32)
        r.abi[...] = jnp.zeros_like(r.abi)

    return dict(clear=clear, d_outer=d_outer, inner_back=inner_back, d_inner=d_inner, first_back=first_back,
                d_output=d_output, att_back=att_back, attention_back=attention_back, d_qkv=d_qkv,
                input_grad=input_grad, small=small)


def backward(x, segc, segr, saved, hu, hi, hp, own):
    hout, hact, hslope, hlow, hob, hsc, hqkv, hatt, inv, lse, vec, acc0 = saved
    seq, dim = x.shape
    ff = hi.shape[1]
    hid = ff // WIDTHS
    rows = dim // 32
    chunks = scatter_chunks(rows, dim, ff) if own else []
    nc = len(chunks)
    extra = ("oq", "ok", "ov", "oo", "oi", "ou", "os") if own else ()
    names = BWD_IN + BWD_OUT + extra + BWD_SCRATCH

    def kernel(*refs):
        r = named(names, refs)
        if own:
            base = len(names)
            sc = Scatter(chunks, (r.gp, r.gi, r.gu), refs[base : base + 5 * nc], refs[base + 5 * nc : -1])
            packed = refs[-1]
            greet(sc.place)
        nsem = [0]

        def load(pairs):
            cps = []
            for a, b in pairs:
                cps.append(pltpu.make_async_copy(a, b, r.sem.at[nsem[0]]))
                nsem[0] += 1
                cps[-1].start()
            return cps

        def wait(cps):
            for cp in cps:
                cp.wait()

        l_ob = load([(r.hob, r.ob), (r.hact, r.act)])
        l_u = load([(r.hu, r.w), (r.hslope, r.slope)])
        l_low = load([(r.hlow, r.low)])
        outs = (r.gp, r.gi, r.gu)
        flying = [None, None]
        turn = [0]

        def emit(a, value, row, col):
            t = turn[0] % 2
            turn[0] += 1
            if flying[t] is not None:
                flying[t].wait()
            nr, ncol = value.shape
            r.stage[t, :, 0:ncol] = value.astype(BF)
            cp = pltpu.make_async_copy(r.stage.at[t, :, pl.ds(0, ncol)],
                                       outs[a].at[pl.ds(row, nr), pl.ds(col, ncol)], r.gsem.at[t])
            cp.start()
            flying[t] = cp

        def flush():
            for t in range(2):
                if flying[t] is not None:
                    flying[t].wait()
                    flying[t] = None

        U, I, O, Q0, Q1 = ((2 * g, 2 * g + 1) for g in range(5))

        def go(group):
            flush()
            if own:
                for ci in group:
                    sc.start(ci)

        def st(n, group):
            if own:
                for ci in group:
                    if n < 4:
                        (sc.stage1, sc.stage2, sc.stage3)[n - 1](ci)
                    else:
                        a, _, r0, nr, c0, ncol, _ = chunks[ci]
                        (packed, r.oi, r.ou)[a][r0 : r0 + nr, c0 : c0 + ncol] = sc.stage4(ci)

        s = bwd_steps(r, emit)
        s["clear"]()
        wait(l_ob)
        for j in range(WIDTHS):
            s["d_outer"](j)
        go(U)
        l_sc = load([(r.hsc, r.act.at[pl.ds(0, 4 * seq), :])])
        wait(l_u)
        s["inner_back"](0, WIDTHS)
        l_i = load([(r.hi.at[:, pl.ds(hid * j, hid)], r.w.at[pl.ds(dim * j, dim), :]) for j in range(WIDTHS)])
        st(1, U)
        wait(l_low)
        for j in range(WIDTHS):
            s["d_inner"](j)
        go(I)
        l_q = load([(r.hqkv, r.low.at[pl.ds(0, 3 * seq), :]), (r.hatt, r.low.at[pl.ds(3 * seq, seq), :])])
        wait(l_sc)
        wait(l_i)
        s["first_back"](3)
        st(2, U)
        s["first_back"](2)
        st(1, I)
        s["first_back"](1)
        st(3, U)
        s["first_back"](0)
        l_p = load([(r.hp.at[:, pl.ds(OUT, dim)], r.w.at[pl.ds(3 * dim, dim), :])])
        l_p2 = load([(r.hp.at[:, pl.ds(3 * HALF * h + HALF * t, HALF)],
                      r.w.at[pl.ds(dim * t, dim), pl.ds(HALF * h, HALF)]) for t in range(3) for h in range(2)])
        wait(l_q)
        s["d_output"]()
        go(O)
        wait(l_p)
        s["att_back"]()
        s["attention_back"](0, 2)
        st(2, I)
        st(1, O)
        s["attention_back"](2, 3)
        s["d_qkv"](0)
        go(Q0)
        st(4, U)
        s["attention_back"](3, 5)
        st(3, I)
        st(2, O)
        st(1, Q0)
        s["attention_back"](5, 6)
        s["d_qkv"](1)
        s["small"]()
        go(Q1)
        st(3, O)
        wait(l_p2)
        s["input_grad"]()
        st(1, Q1)
        st(4, I)
        st(2, Q0)
        st(4, O)
        st(2, Q1)
        st(3, Q0)
        st(3, Q1)
        st(4, Q0)
        st(4, Q1)
        if own:
            for t, ref in enumerate((r.oq, r.ok, r.ov)):
                for h in range(2):
                    at = 3 * HALF * h + HALF * t
                    ref[:, HALF * h : HALF * (h + 1)] = packed[:, at : at + HALF]
            r.oo[...] = packed[:, OUT : OUT + dim]
            r.os[...] = packed[:, SMALL:OUT]
            for ci in range(nc):
                sc.finish(ci)

    any_ = pl.BlockSpec(memory_space=pl.ANY)
    vm = pl.BlockSpec(memory_space=pltpu.VMEM)
    S = jax.ShapeDtypeStruct
    V = pltpu.VMEM
    flat = lambda a: a.reshape(-1, a.shape[-1])
    out_shape = [S((seq, dim), F32), S(hp.shape, BF), S(hi.shape, BF), S(hu.shape, BF)]
    scratch = [V((4 * seq, dim), BF), V((10 * seq, hid), BF), V((10 * seq, hid), BF), V((4 * seq, dim), BF),
               V((ff, dim), BF), V((seq, dim), F32), V((24, dim), F32), V((8, dim), F32),
               V((2, dim // 2, dim), BF), pltpu.SemaphoreType.DMA((24,)), pltpu.SemaphoreType.DMA((2,))]
    params = dict(vmem_limit_bytes=67043328)
    if own:
        out_shape += [S((rows, dim), F32)] * 4 + [S((rows, ff), F32), S((4 * rows, dim), F32), S((rows, EXTRA), F32)]
        for count in (16, 16, 8, 4, 3):
            scratch += [V((count, c[3], c[5]), BF) for c in chunks]
        scratch += [pltpu.SemaphoreType.DMA((nc, k)) for k in (16, 16, 16, 8, 8, 4, 4, 3, 3)]
        scratch += [V((rows, hp.shape[1]), F32)]
        params.update(collective_id=2, has_side_effects=True)
    return pl.pallas_call(
        kernel,
        out_shape=out_shape,
        in_specs=[vm] * 7 + [any_] * 10,
        out_specs=[vm, any_, any_, any_] + [vm] * len(extra),
        scratch_shapes=scratch,
        compiler_params=pltpu.CompilerParams(**params),
        name="backward",
    )(x, segc, segr, inv, lse, vec, acc0, flat(hob), flat(hact), flat(hslope), flat(hlow), flat(hsc), hu, hi, hp,
      flat(hqkv), hatt)


def settle(arrays):
    n = len(arrays)

    def kernel(*refs):
        for a, b in zip(refs[:n], refs[n:]):
            b[...] = a[...]

    return pl.pallas_call(
        kernel,
        out_shape=[jax.ShapeDtypeStruct(a.shape, a.dtype) for a in arrays],
        in_specs=[pl.BlockSpec(memory_space=pltpu.VMEM)] * n,
        out_specs=[pl.BlockSpec(memory_space=pltpu.VMEM)] * n,
        name="settle",
    )(*arrays)


def direct(rows):
    return lax.axis_size("dp") == 2 and lax.axis_size("fsdp") == 16 and rows % 8 == 0


def per_device(inputs, segments, out_grads, wq, bq, wk, wv, bv, wo, bo, g1, s1, wi, bi, wu, bu, g2, s2):
    rows, dim = wq.shape
    ff = wi.shape[1]
    per = ff // dim
    small = jnp.stack([bq, bv, bo, g1, s1, bu, g2, s2], axis=1)
    small = jnp.concatenate([small, bi.reshape(rows, per), jnp.zeros((rows, EXTRA - 8 - per), BF)], axis=1)
    cut = [w[:, HALF * h : HALF * (h + 1)] for h in range(2) for w in (wq, wk, wv)]
    packed = jnp.concatenate(cut + [small, wo], axis=1)
    width = packed.shape[1]
    own = direct(rows)
    if own:
        h = 13 * 128
        chunks = [
            (0, rows, 0, rows, 0, h, 0), (0, rows, 0, rows, h, width - h, 1),
            (1, rows, 0, rows, 0, ff // 2, 0), (1, rows, 0, rows, ff // 2, ff // 2, 1),
            (2, 4 * rows, 0, 2 * rows, 0, dim, 0), (2, 4 * rows, 2 * rows, 2 * rows, 0, dim, 1),
        ]
        full, wi_f, wu_f = gather([packed, wi, wu], chunks, 1)
    else:
        full, wi_f, wu_f = [lax.all_gather(a, AXES, axis=0, tiled=True) for a in (packed, wi, wu)]
    x = inputs[0]
    seg = segments[0]
    segc, segr = seg[:, None], seg[None, :]
    saved = forward(x, segc, segr, out_grads[:, 0], full, wi_f, wu_f)
    done = backward(x, segc, segr, saved, wu_f, wi_f, full, own)
    x_grad = done[0]
    if own:
        x_grad, gq, gk, gv, go, gi, gu, rs = settle([x_grad] + list(done[4:]))
    else:
        red, gi, gu = [lax.psum_scatter(a, AXES, scatter_dimension=0, tiled=True).astype(F32) for a in done[1:4]]
        gq, gk, gv = [
            jnp.concatenate([red[:, 3 * HALF * h + HALF * t :][:, :HALF] for h in range(2)], axis=1) for t in range(3)
        ]
        rs, go = red[:, SMALL:OUT], red[:, OUT:]
    vecs = [rs[:, i] for i in range(8)]
    gb = rs[:, 8 : 8 + per].reshape(-1)
    return (saved[0][:, None], x_grad[None], gq, vecs[0], gk, gv, vecs[1], go, vecs[2], vecs[3], vecs[4], gi, gb, gu,
            vecs[5], vecs[6], vecs[7])


def solution(mesh):
    mat = P(AXES, None)
    vec = P(AXES)
    params = (mat, vec, mat, mat, vec, mat, vec, vec, vec, mat, vec, mat, vec, vec, vec)
    return jax.shard_map(
        per_device,
        mesh=mesh,
        in_specs=(P(AXES, None, None), P(AXES, None), P(None, AXES, None, None)) + params,
        out_specs=(P(None, AXES, None, None), P(AXES, None, None)) + params,
        check_vma=False,
    )
```
